32 devices in a mesh: fsdp: 8 (over z, y), rep: 4 (over x, core).
Axes of the slice: x: 2, y: 2, z: 4, core: 2. Of those that a mesh axis runs over, the one named last changes fastest.
Arguments:
- hidden: bfloat16 [8192, 2048], P(('fsdp', 'rep')), may hold values from -6 to 6
- attn_gain: bfloat16 [2048], P(('fsdp', 'rep')), may hold values from 0.25 to 1.75
- w_query: bfloat16 [2048, 2048], P(('fsdp', 'rep')), as said below
- w_key: bfloat16 [2048, 512], P(('fsdp', 'rep')), as said below
- w_value: bfloat16 [2048, 512], P(('fsdp', 'rep')), may hold values from -0.125 to 0.125
- w_out: bfloat16 [2048, 2048], P(None, ('fsdp', 'rep')), may hold values from -0.125 to 0.125
Outputs:
- mixed: bfloat16 [8192, 2048], P(('fsdp', 'rep'))
The draws below stay inside these ranges and needn't reach their ends.
Inputs may be any that keep to these rules, and one draw needn't show every extreme that they name: `w_query`: entries of order 2048^(-1/2). `w_key`: entries of order 2048^(-1/2) times a factor up to twenty.
All inputs are finite; a program needn't handle non-finite values.
Results may differ from the reference program's by a relative error of at most 0.012.
The reference program's roundings to bfloat16 on the way (of `normed`, `probs` and `context`) count: a program that leaves them out, or rounds other values in their place, can miss the bound.
Values may be sent and summed in bfloat16 or wider, within the bound.
A program may use at most 64 MiB of HBM per device.

```python
import math
import jax
import jax.numpy as jnp
from jax import lax

D = 2048
HEADS = 32
KV_HEADS = 8
HD = 64
TOK_DEV = 256
TOKENS = 8192
N_FSDP = 8
N_REP = 4


def shared_base(key):
    return jax.random.normal(jax.random.fold_in(key, 7), (D, KV_HEADS, 1, HD), jnp.float32) / math.sqrt(D)


def draw_w_query(key, part):
    group = HEADS // KV_HEADS
    others = jax.random.normal(jax.random.fold_in(key, 11), (D, KV_HEADS, group, HD), jnp.float32) / math.sqrt(D)
    joined = jnp.concatenate([shared_base(key), others[:, :, 1:, :]], axis=2)
    return joined.reshape(D, HEADS * HD).astype(jnp.bfloat16)


def draw_w_key(key, part):
    noise = jax.random.normal(jax.random.fold_in(key, 13), (D, KV_HEADS * HD), jnp.float32) / math.sqrt(D)
    result = noise
    return result.astype(jnp.bfloat16)


def block_levels(stream_key, extent, shards, least, high):
    def one(dim, parts):
        draws = jax.random.uniform(jax.random.fold_in(jax.random.fold_in(stream_key, 6), dim), (parts,), jnp.float32, least / len(shards), high / len(shards))
        return jnp.repeat(jnp.exp(draws), extent[dim] // parts).reshape((-1,) + (1,) * (len(extent) - dim - 1))

    level = one(*shards[0])
    for cut in shards[1:]:
        level = level * one(*cut)
    return level


def normal_values(key, extent, spread, most, split=(), held_as=jnp.bfloat16):
    values = jax.random.normal(key, extent, jnp.float32) * spread
    if len(split) > 0:
        values = block_levels(key, extent, split, -0.22, 0.18) * values
    return jnp.clip(values, min=-most, max=most).astype(held_as)


def setup_inputs(seed: int = 0) -> dict:
    streams_of = jax.random.split(jax.random.key(seed), 7)
    return {
        "hidden": normal_values(streams_of[0], (TOKENS, D), 1.0, 6.0, ((0, 32),)),
        "attn_gain": jnp.clip(1.0 + 0.15 * jax.random.normal(streams_of[1], (D,), jnp.float32), 0.25, 1.75).astype(jnp.bfloat16),
        "w_query": draw_w_query(jax.random.fold_in(streams_of[6], 71), 0),
        "w_key": draw_w_key(jax.random.fold_in(streams_of[6], 71), 0),
        "w_value": normal_values(streams_of[4], (D, KV_HEADS * HD), D ** -0.5, 0.125, ((0, 32),)),
        "w_out": normal_values(streams_of[5], (HEADS * HD, D), (HEADS * HD) ** -0.5, 0.125, ((1, 32),)),
    }


rope_base = 500000.0
norm_eps = 1e-05

def rope_tables(tokens, head_dim):
    position = jnp.arange(tokens, dtype=jnp.float32)
    freq = rope_base ** (-(jnp.arange(head_dim // 2, dtype=jnp.float32) * 2.0) / head_dim)
    angle = position[:, None] * freq[None, :]
    cos_table = jnp.concatenate([jnp.cos(angle), jnp.cos(angle)], axis=-1)
    sin_table = jnp.concatenate([jnp.sin(angle), jnp.sin(angle)], axis=-1)
    return (cos_table, sin_table)

def rotate(tensor, cos_table, sin_table):
    half = tensor.shape[-1] // 2
    turned = jnp.concatenate([-tensor[..., half:], tensor[..., :half]], axis=-1)
    return tensor * cos_table + turned * sin_table

def reference(hidden, attn_gain, w_query, w_key, w_value, w_out):
    group = HEADS // KV_HEADS
    cos_table, sin_table = rope_tables(TOK_DEV, HD)
    causal = jnp.arange(TOK_DEV)[:, None] >= jnp.arange(TOK_DEV)[None, :]

    def one_sequence(block):
        x_float = block.astype(jnp.float32)
        inv_rms = lax.rsqrt(lax.optimization_barrier(jnp.mean(x_float * x_float, axis=-1, keepdims=True)) + norm_eps)
        normed = (x_float * inv_rms * attn_gain.astype(jnp.float32)[None, :]).astype(jnp.bfloat16)
        queries = jnp.dot(normed, w_query, preferred_element_type=jnp.float32)
        keys_raw = jnp.dot(normed, w_key, preferred_element_type=jnp.float32)
        values_raw = jnp.dot(normed, w_value, preferred_element_type=jnp.float32)
        queries = queries.reshape(TOK_DEV, KV_HEADS, group, HD)
        keys_raw = keys_raw.reshape(TOK_DEV, KV_HEADS, HD)
        values_bf = values_raw.reshape(TOK_DEV, KV_HEADS, HD).astype(jnp.bfloat16)
        rope_queries = rotate(queries, cos_table[:, None, None, :], sin_table[:, None, None, :]).astype(jnp.bfloat16)
        rope_keys = rotate(keys_raw, cos_table[:, None, :], sin_table[:, None, :]).astype(jnp.bfloat16)
        scores = jnp.einsum('qkgd,skd->kgqs', rope_queries.astype(jnp.float32), rope_keys.astype(jnp.float32)) * HD ** (-0.5)
        scores = jnp.where(causal[None, None, :, :], scores, -1e+30)
        top = lax.optimization_barrier(jnp.max(scores, axis=-1, keepdims=True))
        expo = jnp.exp(scores - top)
        probs = (expo / lax.optimization_barrier(jnp.sum(expo, axis=-1, keepdims=True))).astype(jnp.bfloat16)
        context = jnp.einsum('kgqs,skd->qkgd', probs.astype(jnp.float32), values_bf.astype(jnp.float32))
        context = context.reshape(TOK_DEV, HEADS * HD).astype(jnp.bfloat16)
        return (x_float + jnp.dot(context, w_out, preferred_element_type=jnp.float32)).astype(jnp.bfloat16)
    blocks = hidden.reshape(N_FSDP * N_REP, TOK_DEV, D)
    return lax.map(one_sequence, blocks).reshape(TOKENS, D)
```

```python
import functools

import jax
import jax.numpy as jnp
import numpy as np
from jax import lax
from jax.experimental import pallas as pl
from jax.experimental.pallas import tpu as pltpu
from jax.sharding import PartitionSpec as P

HD = 64
LANES = 128
GROUPS = 2
Z_LINE = 4

rope_base = 500000.0
norm_eps = 1e-05

MESH = pl.DeviceIdType.MESH
NT = (((1,), (1,)), ((), ()))


def rope_tables(tokens, head_dim):
    position = jnp.arange(tokens, dtype=jnp.float32)
    freq = rope_base ** (-(jnp.arange(head_dim // 2, dtype=jnp.float32) * 2.0) / head_dim)
    angle = position[:, None] * freq[None, :]
    cos_table = jnp.concatenate([jnp.cos(angle), jnp.cos(angle)], axis=-1)
    sin_table = jnp.concatenate([jnp.sin(angle), jnp.sin(angle)], axis=-1)
    return (cos_table, sin_table)


def rotate(tensor, cos_table, sin_table):
    half = tensor.shape[-1] // 2
    turned = jnp.concatenate([-tensor[..., half:], tensor[..., :half]], axis=-1)
    return tensor * cos_table + turned * sin_table


def lane_tables(tokens):
    lane = np.arange(LANES)
    freq = np.float64(rope_base) ** (-(lane % (HD // 2)) * 2.0 / HD)
    angle = np.arange(tokens)[:, None] * freq[None, :]
    sign = np.where(lane % HD < HD // 2, -1.0, 1.0)
    return np.cos(angle).astype(np.float32), (np.sin(angle) * sign).astype(np.float32)


def nearest(p, step):
    middle = jnp.where((p == 1) | (p == 2), 1, 0)
    high = step // 2
    low = step % 2
    low = low + middle * high * (1 - 2 * low)
    first = (1 - 2 * (p % 2)) * low
    return p + first + (2 - 4 * (p // 2)) * high


def block_kernel(
    hid_hbm, gain_hbm, wq_hbm, wk_hbm, wv_hbm, wo_hbm, cos_hbm, sin_hbm, out_hbm,
    wa, wv, wo, hid, nrm, acc, ctx, cos_ref, sin_ref, psend, precv, own, outv,
    origin_sem, send_sem, recv_sem, sib_sem, xsend_sem, xrecv_sem, local_sem,
    psend_sem, precv_sem, out_sem,
):
    f, r = lax.axis_index("fsdp"), lax.axis_index("rep")
    z, y = f // 2, f % 2
    x, c = r // 2, r % 2
    tokens, width = hid.shape[1], hid.shape[2]
    rows = wa.shape[4]
    qw = wq_hbm.shape[1] // 2 // GROUPS
    kw = wk_hbm.shape[1] // 2 // GROUPS
    half_out = wo.shape[4]
    cut = half_out - LANES
    span = width // Z_LINE
    partner = (f, (1 - x) * 2 + c)
    sibling = (f, x * 2 + 1 - c)
    across = (z * 2 + 1 - y, r)
    up = (f + 2, r)
    down = (f - 2, r)
    has_up = z + 1 < Z_LINE
    has_down = z >= 1

    def view(kind, g, fs, which):
        if kind == "a":
            return wa.at[g, fs, :, which]
        if kind == "b":
            return wv.at[g, fs, :, which]
        if kind == "oa":
            return wo.at[fs, :, which, :, pl.ds(0, cut)]
        return wo.at[fs, :, which, :, pl.ds(cut, LANES)]

    def index(kind, g):
        return {"a": g, "b": GROUPS + g, "oa": 2 * GROUPS, "ob": 2 * GROUPS + 1}[kind]

    targets = {"up": (0, up, has_up), "down": (1, down, has_down), "across": (2, across, None),
               "sibling": (3, sibling, None)}

    def remote(kind, g, fs, way):
        number, target, _ = targets[way]
        k = index(kind, g)
        ref = view(kind, g, fs, c)
        arrive = sib_sem if way == "sibling" else recv_sem
        return pltpu.make_async_remote_copy(
            src_ref=ref, dst_ref=ref, send_sem=send_sem.at[k, fs, number],
            recv_sem=arrive.at[k, fs], device_id=target, device_id_type=MESH)

    def origin(kind, g, xs, way):
        number, target, _ = targets[way]
        k = index(kind, g)
        ref = view(kind, g, f, c).at[xs]
        arrive = sib_sem if way == "sibling" else recv_sem
        return pltpu.make_async_remote_copy(
            src_ref=ref, dst_ref=ref, send_sem=origin_sem.at[k, xs, number],
            recv_sem=arrive.at[k, f], device_id=target, device_id_type=MESH)

    def when(cond, act):
        if cond is None:
            act()
        else:
            pl.when(cond)(act)

    def spread_origin(kinds, g, xs, act):
        for kind in kinds:
            for way in ("up", "down", "across", "sibling"):
                when(targets[way][2], lambda kind=kind, way=way: act(origin(kind, g, xs, way)))

    def away(kind, g, fs, zs, act):
        when((zs <= z) & has_up, lambda: act(remote(kind, g, fs, "up")))
        when((zs >= z) & has_down, lambda: act(remote(kind, g, fs, "down")))

    def start(copy):
        copy.start()

    def finish(copy):
        copy.wait_send()

    def arrived(kind, g, fs):
        remote(kind, g, fs, "across").wait_recv()

    def near_step(main, side, g, s):
        zs = nearest(z, s)

        @pl.when(s > 0)
        def _():
            fs = zs * 2 + y
            arrived(main, g, fs)
            away(main, g, fs, zs, start)
            remote(main, g, fs, "across").start()
            remote(main, g, fs, "sibling").start()
            arrived(side, g, fs)
            away(side, g, fs, zs, start)
            remote(side, g, fs, "sibling").start()

        fo = zs * 2 + 1 - y
        arrived(side, g, fo)
        away(side, g, fo, zs, start)
        remote(side, g, fo, "sibling").start()

    def far_step(main, g, s):
        fo = nearest(z, s) * 2 + 1 - y
        arrived(main, g, fo)
        remote(main, g, fo, "sibling").start()

    def near_done(main, side, g, s):
        zs = nearest(z, s)

        @pl.when(s > 0)
        def _():
            fs = zs * 2 + y
            away(main, g, fs, zs, finish)
            remote(main, g, fs, "across").wait_send()
            remote(main, g, fs, "sibling").wait_send()
            away(side, g, fs, zs, finish)
            remote(side, g, fs, "sibling").wait_send()

        fo = zs * 2 + 1 - y
        away(side, g, fo, zs, finish)
        remote(side, g, fo, "sibling").wait_send()
        remote(main, g, fo, "sibling").wait_send()

    def sibling_arrived(kinds, g, s):
        zs = nearest(z, s)
        for kind in kinds:
            for col in range(2):
                fs = zs * 2 + col
                ref = view(kind, g, fs, 1 - c)
                pltpu.make_async_remote_copy(
                    src_ref=ref, dst_ref=ref, send_sem=send_sem.at[index(kind, g), fs, 3],
                    recv_sem=sib_sem.at[index(kind, g), fs], device_id=sibling,
                    device_id_type=MESH).wait_recv()

    def q_cols(h, g):
        return pl.ds(pl.multiple_of((h * GROUPS + g) * qw, LANES), qw)

    def k_cols(h, g):
        return pl.ds(pl.multiple_of((h * GROUPS + g) * kw, LANES), kw)

    def o_cols(h):
        return pl.ds(pl.multiple_of(h * half_out, LANES), half_out)

    def local(src, dst, sem):
        return pltpu.make_async_copy(src, dst, local_sem.at[sem])

    for g in range(GROUPS):
        local(wq_hbm.at[:, q_cols(x, g)], wa.at[g, f, x, c, :, pl.ds(0, qw)], 2 * g).start()
        local(wk_hbm.at[:, k_cols(x, g)], wa.at[g, f, x, c, :, pl.ds(qw, kw)], 2 * g).start()
        local(wv_hbm.at[:, k_cols(x, g)], wv.at[g, f, x, c, pl.ds(0, rows)], 2 * g + 1).start()
        local(gain_hbm, wv.at[g, f, x, c, pl.ds(rows, 16)], 2 * g + 1).start()
    local(wo_hbm.at[:, o_cols(x)], wo.at[f, x, c], 4).start()
    local(hid_hbm, hid.at[0], 5).start()
    local(cos_hbm, cos_ref, 6).start()
    local(sin_hbm, sin_ref, 7).start()

    barrier = pltpu.get_barrier_semaphore()
    for target, cond in ((across, None), (up, has_up), (down, has_down), (partner, None),
                         (sibling, None)):
        when(cond, lambda target=target: pl.semaphore_signal(
            barrier, inc=1, device_id=target, device_id_type=MESH))
    pl.semaphore_wait(barrier, 3 + jnp.where(has_up, 1, 0) + jnp.where(has_down, 1, 0))

    def swap(src, dst, number, sem):
        return pltpu.make_async_remote_copy(
            src_ref=src, dst_ref=dst, send_sem=xsend_sem.at[number], recv_sem=xrecv_sem.at[sem],
            device_id=partner, device_id_type=MESH)

    swaps = []
    for g in range(GROUPS):
        h = 1 - x
        swaps += [
            swap(wq_hbm.at[:, q_cols(h, g)], wa.at[g, f, x, c, :, pl.ds(0, qw)], 4 * g, 2 * g),
            swap(wk_hbm.at[:, k_cols(h, g)], wa.at[g, f, x, c, :, pl.ds(qw, kw)], 4 * g + 1, 2 * g),
            swap(wv_hbm.at[:, k_cols(h, g)], wv.at[g, f, x, c, pl.ds(0, rows)], 4 * g + 2, 2 * g + 1),
            swap(gain_hbm, wv.at[g, f, x, c, pl.ds(rows, 16)], 4 * g + 3, 2 * g + 1),
        ]
    swaps.append(swap(hid_hbm, hid.at[1], 8, 4))
    swaps.append(swap(wo_hbm.at[:, o_cols(1 - x)], wo.at[f, x, c], 9, 5))
    for copy in swaps:
        copy.start()

    def swapped(ref, sem):
        swap(ref, ref, 0, sem).wait_recv()

    for g in range(GROUPS):
        local(wa.at[g, f, x, c], wa.at[g, f, x, c], 2 * g).wait()
        local(wv.at[g, f, x, c], wv.at[g, f, x, c], 2 * g + 1).wait()
        spread_origin(("a", "b"), g, x, start)

    def inverse_rms(t):
        value = hid[t].astype(jnp.float32)
        return lax.rsqrt(jnp.mean(value * value, axis=-1, keepdims=True) + norm_eps)

    def gain_row(zs):
        lane = lax.broadcasted_iota(jnp.int32, (1, LANES), 1)
        parts = []
        for col in range(2):
            for xs in range(2):
                low = wv[0, zs * 2 + col, xs, 0, rows:rows + 16, :].astype(jnp.float32)[0:1]
                high = wv[0, zs * 2 + col, xs, 1, rows:rows + 16, :].astype(jnp.float32)[0:1]
                parts.append(jnp.where(lane < rows, low, high))
        return jnp.concatenate(parts, axis=1)

    def normalize(t, zs, inv):
        cols = pl.ds(pl.multiple_of(zs * span, LANES), span)
        value = hid[t, :, cols].astype(jnp.float32) * inv * gain_row(zs)
        nrm[pl.ds(t * tokens, tokens), cols] = value.astype(jnp.bfloat16)

    def project(t, g, zs):
        cols = pl.ds(pl.multiple_of(zs * span, LANES), span)
        left = nrm[pl.ds(t * tokens, tokens), cols]
        fs = pl.ds(zs * 2, 2)
        weight = jnp.concatenate(
            [wa[g, fs].reshape(span, qw + kw), wv[g, fs, :, :, 0:rows, :].reshape(span, kw)], axis=1)
        acc[g, pl.ds(t * tokens, tokens), :] += jnp.dot(
            left, weight, preferred_element_type=jnp.float32)

    acc[...] = jnp.zeros_like(acc)
    local(hid_hbm, hid.at[0], 5).wait()
    inv_own = inverse_rms(0)

    for g in range(GROUPS):
        swapped(wa.at[g, f, 1 - x, c], 2 * g)
        swapped(wv.at[g, f, 1 - x, c], 2 * g + 1)
        spread_origin(("a", "b"), g, 1 - x, start)

    steps = GROUPS * Z_LINE

    def own_chunk(n):
        g, s = n // Z_LINE, n % Z_LINE
        zs = nearest(z, s)
        sibling_arrived(("a", "b"), g, s)

        @pl.when(g == 0)
        def _():
            normalize(0, zs, inv_own)

        project(0, g, zs)

    def qkv_step(n, carry):
        near_step("a", "b", n // Z_LINE, n % Z_LINE)

        @pl.when(n >= 1)
        def _():
            far_step("a", (n - 1) // Z_LINE, (n - 1) % Z_LINE)

        @pl.when(n >= 2)
        def _():
            own_chunk(n - 2)

        return carry

    lax.fori_loop(0, steps - 1, qkv_step, 0)

    swap(hid_hbm, hid.at[1], 8, 4).wait_recv()
    inv_other = inverse_rms(1)

    def other_first(zs, carry):
        normalize(1, zs, inv_other)
        project(1, 0, zs)
        return carry

    lax.fori_loop(0, Z_LINE, other_first, 0)
    near_step("a", "b", GROUPS - 1, Z_LINE - 1)
    far_step("a", GROUPS - 1, Z_LINE - 2)

    local(wo_hbm.at[:, o_cols(x)], wo.at[f, x, c], 4).wait()
    spread_origin(("oa", "ob"), 0, x, start)
    swapped(wo.at[f, 1 - x, c], 5)
    spread_origin(("oa", "ob"), 0, 1 - x, start)
    own_chunk(steps - 3)

    local(cos_hbm, cos_ref, 6).wait()
    local(sin_hbm, sin_ref, 7).wait()

    def attend(g, t):
        base = pl.multiple_of(t * tokens, tokens)
        span_rows = pl.ds(base, tokens)
        lane = lax.broadcasted_iota(jnp.int32, (tokens, LANES), 1)
        first = lane % HD < HD // 2
        left_head = lane < HD

        def turn(tile):
            turned = jnp.where(first, pltpu.roll(tile, LANES - HD // 2, 1),
                               pltpu.roll(tile, HD // 2, 1))
            return tile * cos_ref[...] + turned * sin_ref[...]

        key = turn(acc[g, span_rows, qw:qw + kw])
        value = acc[g, span_rows, qw + kw:qw + 2 * kw]
        key_other, value_other = pltpu.roll(key, HD, 1), pltpu.roll(value, HD, 1)
        for j in range(kw // HD):
            def low_high(tile, tile_other):
                low = tile if j == 0 else tile_other
                high = tile_other if j == 0 else tile
                zero = jnp.zeros_like(tile)
                return (jnp.where(left_head, low, zero).astype(jnp.bfloat16),
                        jnp.where(left_head, zero, high).astype(jnp.bfloat16))

            key_low, key_high = low_high(key, key_other)
            value_low, value_high = low_high(value, value_other)
            heads = qw // (kw // HD)
            query = []
            for p in range(heads // LANES):
                at = j * heads + p * LANES
                tile = turn(acc[g, span_rows, at:at + LANES])
                query.append(tile.astype(jnp.bfloat16) * jnp.bfloat16(HD ** -0.5))
            block = tokens // 2
            for b in range(2):
                seen = (b + 1) * block
                rows_q = slice(b * block, (b + 1) * block)
                stacked = jnp.concatenate([q[rows_q] for q in query], axis=0)
                keys = jnp.concatenate([key_low[:seen], key_high[:seen]], axis=0)
                values = jnp.concatenate([value_low[:seen], value_high[:seen]], axis=0)
                scores = lax.dot_general(stacked, keys, NT, preferred_element_type=jnp.float32)
                count = stacked.shape[0]
                at_row = lax.broadcasted_iota(jnp.int32, (count, seen), 0) % block + b * block
                at_col = lax.broadcasted_iota(jnp.int32, (count, seen), 1)
                open_ = at_row >= at_col
                probs = []
                for e in range(2):
                    part = jnp.where(open_, scores[:, e * seen:(e + 1) * seen], -1e30)
                    top = jnp.max(part, axis=-1, keepdims=True)
                    expo = jnp.exp(part - top)
                    total = jnp.sum(expo, axis=-1, keepdims=True)
                    probs.append((expo * (1.0 / total)).astype(jnp.bfloat16))
                mixed = jnp.dot(jnp.concatenate(probs, axis=1), values,
                                preferred_element_type=jnp.float32).astype(jnp.bfloat16)
                for p in range(heads // LANES):
                    at = g * qw + j * heads + p * LANES
                    ctx[pl.ds(base + b * block, block), at:at + LANES] = (
                        mixed[p * block:(p + 1) * block])

    def attend_first(t, carry):
        attend(0, t)
        return carry

    lax.fori_loop(0, 2, attend_first, 0)

    far_step("a", GROUPS - 1, Z_LINE - 1)
    own_chunk(steps - 2)
    near_step("oa", "ob", 0, 0)
    own_chunk(steps - 1)

    def other_second(zs, carry):
        project(1, 1, zs)
        return carry

    lax.fori_loop(0, Z_LINE, other_second, 0)
    attend(1, 1)

    def out_weight(s):
        return wo[pl.ds(nearest(z, s) * 2, 2)].reshape(span, half_out)

    def share(s):
        return pltpu.make_async_remote_copy(
            src_ref=psend.at[s], dst_ref=precv.at[s], send_sem=psend_sem.at[s],
            recv_sem=precv_sem.at[s], device_id=partner, device_id_type=MESH)

    def out_other(s):
        part = lax.dot_general(ctx[tokens:2 * tokens, :], out_weight(s), NT,
                               preferred_element_type=jnp.float32)
        psend[s] = part.astype(jnp.bfloat16)
        share(s).start()

    def out_own(s):
        cols = pl.ds(pl.multiple_of(nearest(z, s) * span, LANES), span)
        part = lax.dot_general(ctx[0:tokens, :], out_weight(s), NT,
                               preferred_element_type=jnp.float32)
        own[s] = hid[0, :, cols].astype(jnp.float32) + part

    def emit(s):
        cols = pl.ds(pl.multiple_of(nearest(z, s) * span, LANES), span)
        return pltpu.make_async_copy(outv.at[s], out_hbm.at[:, cols], out_sem.at[s])

    def close(s):
        share(s).wait_recv()
        outv[s] = (own[s] + precv[s].astype(jnp.float32)).astype(jnp.bfloat16)
        emit(s).start()

    far_step("oa", 0, 0)
    sibling_arrived(("oa", "ob"), 0, 0)
    out_other(0)
    near_step("oa", "ob", 0, 1)
    attend(1, 0)
    out_own(0)

    def out_step(s, carry):
        far_step("oa", 0, s)

        @pl.when(s < Z_LINE - 1)
        def _():
            near_step("oa", "ob", 0, s + 1)

        sibling_arrived(("oa", "ob"), 0, s)
        out_other(s)
        out_own(s)
        return carry

    lax.fori_loop(1, Z_LINE, out_step, 0)

    def close_step(s, carry):
        close(s)
        return carry

    lax.fori_loop(0, Z_LINE, close_step, 0)

    for copy in swaps:
        copy.wait_send()
    for g in range(GROUPS):
        for xs in range(2):
            spread_origin(("a", "b"), g, xs, finish)
    for xs in range(2):
        spread_origin(("oa", "ob"), 0, xs, finish)

    def drain_qkv(n, carry):
        near_done("a", "b", n // Z_LINE, n % Z_LINE)
        return carry

    lax.fori_loop(0, steps, drain_qkv, 0)

    def drain_out(s, carry):
        near_done("oa", "ob", 0, s)
        share(s).wait_send()
        emit(s).wait()
        return carry

    lax.fori_loop(0, Z_LINE, drain_out, 0)


def fused(hidden, attn_gain, w_query, w_key, w_value, w_out):
    tokens, width = hidden.shape
    rows, width_query = w_query.shape
    width_kv = w_key.shape[1]
    fsdp = Z_LINE * 2
    qw, kw = width_query // 2 // GROUPS, width_kv // 2 // GROUPS
    half_out = width_query // 2
    span = width // Z_LINE
    gain = jnp.broadcast_to(jnp.concatenate([attn_gain, attn_gain])[None, :], (16, LANES))
    cos_table, sin_table = lane_tables(tokens)
    kinds = 2 * GROUPS + 2
    dma = pltpu.SemaphoreType.DMA
    return pl.pallas_call(
        block_kernel,
        out_shape=jax.ShapeDtypeStruct((tokens, width), hidden.dtype),
        in_specs=[pl.BlockSpec(memory_space=pl.ANY)] * 8,
        out_specs=pl.BlockSpec(memory_space=pl.ANY),
        scratch_shapes=[
            pltpu.VMEM((GROUPS, fsdp, 2, 2, rows, qw + kw), jnp.bfloat16),
            pltpu.VMEM((GROUPS, fsdp, 2, 2, rows + 16, kw), jnp.bfloat16),
            pltpu.VMEM((fsdp, 2, 2, rows, half_out), jnp.bfloat16),
            pltpu.VMEM((2, tokens, width), jnp.bfloat16),
            pltpu.VMEM((2 * tokens, width), jnp.bfloat16),
            pltpu.VMEM((GROUPS, 2 * tokens, qw + 2 * kw), jnp.float32),
            pltpu.VMEM((2 * tokens, half_out), jnp.bfloat16),
            pltpu.VMEM((tokens, LANES), jnp.float32),
            pltpu.VMEM((tokens, LANES), jnp.float32),
            pltpu.VMEM((Z_LINE, tokens, span), jnp.bfloat16),
            pltpu.VMEM((Z_LINE, tokens, span), jnp.bfloat16),
            pltpu.VMEM((Z_LINE, tokens, span), jnp.float32),
            pltpu.VMEM((Z_LINE, tokens, span), jnp.bfloat16),
            dma((kinds, 2, 4)),
            dma((kinds, fsdp, 4)),
            dma((kinds, fsdp)),
            dma((kinds, fsdp)),
            dma((10,)),
            dma((6,)),
            dma((8,)),
            dma((Z_LINE,)),
            dma((Z_LINE,)),
            dma((Z_LINE,)),
        ],
        compiler_params=pltpu.CompilerParams(
            collective_id=0, has_side_effects=True, vmem_limit_bytes=60 * 1024 * 1024),
        name="attention_block",
    )(hidden, gain, w_query, w_key, w_value, w_out.T, jnp.asarray(cos_table), jnp.asarray(sin_table))


def fits(fsdp, rep, hidden, w_query, w_key, w_out):
    tokens, width = hidden.shape
    rows, width_query = w_query.shape
    return (
        rep == 4
        and fsdp == 2 * Z_LINE
        and 2 * rows == LANES
        and width == fsdp * rep * rows
        and w_out.shape == (width_query, rows)
        and w_key.shape[1] == 2 * GROUPS * LANES
        and width_query == 4 * w_key.shape[1]
        and tokens % LANES == 0
    )


def body(fsdp, rep, hidden, attn_gain, w_query, w_key, w_value, w_out):
    if fits(fsdp, rep, hidden, w_query, w_key, w_out):
        return fused(hidden, attn_gain, w_query, w_key, w_value, w_out)
    tokens = hidden.shape[0]
    head_dim = HD
    width_query = w_query.shape[1]
    width_kv = w_key.shape[1]
    kv_count = width_kv // head_dim
    group = width_query // width_kv
    x_float = hidden.astype(jnp.float32)
    inv_rms = lax.rsqrt(jnp.mean(x_float * x_float, axis=-1, keepdims=True) + norm_eps)
    width_rows = w_query.shape[0]
    packed = jnp.concatenate(
        [w_query, w_key, w_value, w_out.T, jnp.broadcast_to(attn_gain[:, None], (width_rows, 128))],
        axis=1,
    )
    packed = lax.all_gather(packed, ("fsdp", "rep"), axis=0, tiled=True)
    cut_key = width_query
    cut_value = cut_key + width_kv
    cut_out = cut_value + width_kv
    cut_gain = cut_out + w_out.shape[0]
    query_piece = packed[:, :cut_key]
    key_piece = packed[:, cut_key:cut_value]
    value_piece = packed[:, cut_value:cut_out]
    out_piece = packed[:, cut_out:cut_gain]
    gain_piece = packed[:, cut_gain]
    normed = (x_float * inv_rms * gain_piece.astype(jnp.float32)[None, :]).astype(jnp.bfloat16)
    queries = jnp.dot(normed, query_piece, preferred_element_type=jnp.float32)
    keys_raw = jnp.dot(normed, key_piece, preferred_element_type=jnp.float32)
    values_raw = jnp.dot(normed, value_piece, preferred_element_type=jnp.float32)
    cos_table, sin_table = rope_tables(tokens, head_dim)
    queries = queries.reshape(tokens, kv_count, group, head_dim)
    keys_raw = keys_raw.reshape(tokens, kv_count, head_dim)
    values_bf = values_raw.reshape(tokens, kv_count, head_dim).astype(jnp.bfloat16)
    rope_queries = rotate(queries, cos_table[:, None, None, :], sin_table[:, None, None, :]).astype(
        jnp.bfloat16
    )
    rope_keys = rotate(keys_raw, cos_table[:, None, :], sin_table[:, None, :]).astype(jnp.bfloat16)
    scores = jnp.einsum(
        "qkgd,skd->kgqs", rope_queries, rope_keys, preferred_element_type=jnp.float32
    ) * head_dim ** (-0.5)
    causal = jnp.arange(tokens)[:, None] >= jnp.arange(tokens)[None, :]
    scores = jnp.where(causal[None, None, :, :], scores, -1e30)
    top = jnp.max(scores, axis=-1, keepdims=True)
    expo = jnp.exp(scores - top)
    probs = (expo / jnp.sum(expo, axis=-1, keepdims=True)).astype(jnp.bfloat16)
    context = jnp.einsum("kgqs,skd->qkgd", probs, values_bf, preferred_element_type=jnp.float32)
    context = context.reshape(tokens, width_query).astype(jnp.bfloat16)
    branch = lax.dot_general(
        context, out_piece, (((1,), (1,)), ((), ())), preferred_element_type=jnp.float32
    )
    return (x_float + branch).astype(jnp.bfloat16)


def solution(mesh):
    placed = (
        P(("fsdp", "rep"), None),
        P(("fsdp", "rep")),
        P(("fsdp", "rep"), None),
        P(("fsdp", "rep"), None),
        P(("fsdp", "rep"), None),
        P(None, ("fsdp", "rep")),
    )
    return jax.shard_map(
        functools.partial(body, mesh.shape["fsdp"], mesh.shape["rep"]),
        mesh=mesh,
        in_specs=placed,
        out_specs=P(("fsdp", "rep"), None),
        check_vma=False,
    )
```

```python
import functools

import jax
import jax.numpy as jnp
import numpy as np
from jax import lax
from jax.experimental import pallas as pl
from jax.experimental.pallas import tpu as pltpu
from jax.sharding import PartitionSpec as P

HD = 64
LANES = 128
GROUPS = 2
Z_LINE = 4

rope_base = 500000.0
norm_eps = 1e-05

MESH = pl.DeviceIdType.MESH
NT = (((1,), (1,)), ((), ()))

PIECES = (("a", 0), ("a", 1), ("b", 0), ("b", 1), ("oa", 0), ("ob", 0))
EDGE_PLAN = (
    (100, 102, 101, 103, 1, 20, 9, 17, 28, 2, 4, 5, 13, 3, 22,),
    (21, 26, 18, 12, 6,),
    (25, 104, 7, 19,),
    (23,),
    (10,),
    (),
    (),
    (11, 29,),
    (27, 105, 14,),
    (),
    (),
    (30, 15,),
    (31,),
    (),
    (36,),
    (44, 33,),
    (),
    (34, 41,),
    (45, 37,),
    (),
    (),
    (),
    (),
    (35, 38, 46,),
    (42,),
    (47,),
    (43, 39,),
    (),
    (),
    (),
    (),
    (),
    (),
    (),
)
MIDDLE_PLAN = (
    (100, 102, 101, 103, 0, 21, 16, 5, 18, 2, 20, 3, 24, 23,),
    (13, 6, 22, 26, 19, 4, 8, 10,),
    (),
    (28, 7,),
    (11,),
    (27, 12, 29, 14,),
    (104,),
    (),
    (),
    (30, 31, 105,),
    (),
    (15,),
    (),
    (32, 34,),
    (37, 45,),
    (),
    (40,),
    (44,),
    (),
    (35,),
    (46, 36,),
    (42,),
    (),
    (47, 43, 38,),
    (),
    (),
    (39,),
    (),
    (),
    (),
    (),
    (),
    (),
    (),
)


def rope_tables(tokens, head_dim):
    position = jnp.arange(tokens, dtype=jnp.float32)
    freq = rope_base ** (-(jnp.arange(head_dim // 2, dtype=jnp.float32) * 2.0) / head_dim)
    angle = position[:, None] * freq[None, :]
    cos_table = jnp.concatenate([jnp.cos(angle), jnp.cos(angle)], axis=-1)
    sin_table = jnp.concatenate([jnp.sin(angle), jnp.sin(angle)], axis=-1)
    return (cos_table, sin_table)


def rotate(tensor, cos_table, sin_table):
    half = tensor.shape[-1] // 2
    turned = jnp.concatenate([-tensor[..., half:], tensor[..., :half]], axis=-1)
    return tensor * cos_table + turned * sin_table


def lane_tables(tokens):
    lane = np.arange(LANES)
    freq = np.float64(rope_base) ** (-(lane % (HD // 2)) * 2.0 / HD)
    angle = np.arange(tokens)[:, None] * freq[None, :]
    sign = np.where(lane % HD < HD // 2, -1.0, 1.0)
    return np.cos(angle).astype(np.float32), (np.sin(angle) * sign).astype(np.float32)


def nearest(p, step):
    middle = jnp.where((p == 1) | (p == 2), 1, 0)
    high = step // 2
    low = step % 2
    low = low + middle * high * (1 - 2 * low)
    first = (1 - 2 * (p % 2)) * low
    return p + first + (2 - 4 * (p // 2)) * high


def block_kernel(
    hid_hbm, gain_hbm, wq_hbm, wk_hbm, wv_hbm, wo_hbm, cos_hbm, sin_hbm, out_ref,
    wa, wv, woa, wob, hid, nrm, acc, ctx, cos_ref, sin_ref, psend, precv, own, gain_in, gain_tile,
    origin_sem, send_sem, recv_sem, sib_sem, xsend_sem, xrecv_sem, local_sem,
    psend_sem, precv_sem,
):
    f, r = lax.axis_index("fsdp"), lax.axis_index("rep")
    z, y = f // 2, f % 2
    x, c = r // 2, r % 2
    tokens, width = hid.shape[1], hid.shape[2]
    rows = wa.shape[4]
    qw = wq_hbm.shape[1] // 2 // GROUPS
    kw = wk_hbm.shape[1] // 2 // GROUPS
    cut = woa.shape[4]
    half_out = cut + wob.shape[4]
    span = width // Z_LINE
    partner = (f, (1 - x) * 2 + c)
    sibling = (f, x * 2 + 1 - c)
    across = (z * 2 + 1 - y, r)
    low_half = z < Z_LINE // 2
    edge = (z == 0) | (z == Z_LINE - 1)
    middle = jnp.logical_not(edge)
    toward = jnp.where(low_half, 2, -2)
    outward = (f - toward, r)
    inward = (f + toward, r)
    mine = jnp.where(edge, 0, 1)

    def at_line(k):
        return jnp.where(low_half, k, Z_LINE - 1 - k)

    def view(kind, g, fs, which):
        if kind == "a":
            return wa.at[g, fs, :, which]
        if kind == "b":
            return wv.at[g, fs, :, which]
        if kind == "oa":
            return woa.at[fs, :, which]
        return wob.at[fs, :, which]

    def index(kind, g):
        return {"a": g, "b": GROUPS + g, "oa": 2 * GROUPS, "ob": 2 * GROUPS + 1}[kind]

    targets = {"outward": (0, outward), "inward": (1, inward), "across": (2, across),
               "sibling": (3, sibling)}

    def remote(kind, g, fs, way):
        number, target = targets[way]
        k = index(kind, g)
        ref = view(kind, g, fs, c)
        arrive = sib_sem if way == "sibling" else recv_sem
        return pltpu.make_async_remote_copy(
            src_ref=ref, dst_ref=ref, send_sem=send_sem.at[k, fs, number],
            recv_sem=arrive.at[k, fs], device_id=target, device_id_type=MESH)

    def origin(kind, g, xs, way):
        number, target = targets[way]
        k = index(kind, g)
        ref = view(kind, g, f, c).at[xs]
        arrive = sib_sem if way == "sibling" else recv_sem
        return pltpu.make_async_remote_copy(
            src_ref=ref, dst_ref=ref, send_sem=origin_sem.at[k, xs, number],
            recv_sem=arrive.at[k, f], device_id=target, device_id_type=MESH)

    def relay(piece, own):
        kind, g = PIECES[piece // 8]
        col, k = piece // 4 % 2, piece % 4
        main = kind in ("a", "oa")
        fs = at_line(k) * 2 + (y if col == 0 else 1 - y)
        remote(kind, g, fs, "across").wait_recv()
        if not (main and col == 1):
            if k >= own and own > 0:
                remote(kind, g, fs, "outward").start()
            if k <= own:
                remote(kind, g, fs, "inward").start()
            if main and col == 0:
                remote(kind, g, fs, "across").start()
        remote(kind, g, fs, "sibling").start()

    def sent(kind, g, k):
        main = kind in ("a", "oa")
        out_ok, in_ok = middle & (k >= mine), k <= mine

        def column(col, side):
            fs = at_line(k) * 2 + (y if col == 0 else 1 - y)
            if side:
                pl.when(out_ok)(lambda: remote(kind, g, fs, "outward").wait_send())
                pl.when(in_ok)(lambda: remote(kind, g, fs, "inward").wait_send())
            if main and col == 0:
                remote(kind, g, fs, "across").wait_send()
            remote(kind, g, fs, "sibling").wait_send()

        pl.when(k != mine)(lambda: column(0, True))
        column(1, not main)

    def origin_ways(kinds, g, xs, act, middle_chip):
        for kind in kinds:
            for way in targets:
                if way == "outward":
                    if middle_chip is True:
                        act(origin(kind, g, xs, way))
                    elif middle_chip is not False:
                        pl.when(middle_chip)(lambda kind=kind: act(origin(kind, g, xs, "outward")))
                else:
                    act(origin(kind, g, xs, way))

    def start(copy):
        copy.start()

    def finish(copy):
        copy.wait_send()

    def sibling_arrived(kinds, g, s):
        zs = nearest(z, s)
        for kind in kinds:
            for col in range(2):
                fs = zs * 2 + col
                ref = view(kind, g, fs, 1 - c)
                pltpu.make_async_remote_copy(
                    src_ref=ref, dst_ref=ref, send_sem=send_sem.at[index(kind, g), fs, 3],
                    recv_sem=sib_sem.at[index(kind, g), fs], device_id=sibling,
                    device_id_type=MESH).wait_recv()

    def q_cols(h, g):
        return pl.ds(pl.multiple_of((h * GROUPS + g) * qw, LANES), qw)

    def k_cols(h, g):
        return pl.ds(pl.multiple_of((h * GROUPS + g) * kw, LANES), kw)

    def oa_cols(h):
        return pl.ds(pl.multiple_of(h * half_out, LANES), cut)

    def ob_cols(h):
        return pl.ds(pl.multiple_of(h * half_out + cut, LANES), half_out - cut)

    def local(src, dst, sem):
        return pltpu.make_async_copy(src, dst, local_sem.at[sem])

    local(gain_hbm, gain_in, 9).start()
    for g in range(GROUPS):
        local(wq_hbm.at[:, q_cols(x, g)], wa.at[g, f, x, c, :, pl.ds(0, qw)], 2 * g).start()
        local(wk_hbm.at[:, k_cols(x, g)], wa.at[g, f, x, c, :, pl.ds(qw, kw)], 2 * g).start()
        local(wv_hbm.at[:, k_cols(x, g)], wv.at[g, f, x, c, pl.ds(0, rows)], 2 * g + 1).start()
    local(wo_hbm.at[:, oa_cols(x)], woa.at[f, x, c], 4).start()
    local(wo_hbm.at[:, ob_cols(x)], wob.at[f, x, c], 5).start()
    local(hid_hbm, hid.at[0], 6).start()
    local(cos_hbm, cos_ref, 7).start()
    local(sin_hbm, sin_ref, 8).start()

    def inverse_rms(t):
        value = hid[t].astype(jnp.float32)
        return lax.rsqrt(jnp.mean(value * value, axis=-1, keepdims=True) + norm_eps)

    barrier = pltpu.get_barrier_semaphore()
    for target in (across, inward, partner, sibling):
        pl.semaphore_signal(barrier, inc=1, device_id=target, device_id_type=MESH)
    pl.when(middle)(lambda: pl.semaphore_signal(
        barrier, inc=1, device_id=outward, device_id_type=MESH))
    acc[...] = jnp.zeros_like(acc)
    local(gain_hbm, gain_in, 9).wait()
    gain = gain_in[...].astype(jnp.float32)
    gain = jnp.broadcast_to(jnp.concatenate([gain, gain], axis=1), (16, LANES))
    gain_tile[...] = gain.astype(jnp.bfloat16)
    for g in range(GROUPS):
        wv[g, f, x, c, rows:rows + 16, :] = gain.astype(jnp.bfloat16)
    local(hid_hbm, hid.at[0], 6).wait()
    inv_own = inverse_rms(0)
    pl.semaphore_wait(barrier, 4 + mine)

    def swap(src, dst, number, sem):
        return pltpu.make_async_remote_copy(
            src_ref=src, dst_ref=dst, send_sem=xsend_sem.at[number], recv_sem=xrecv_sem.at[sem],
            device_id=partner, device_id_type=MESH)

    swaps = []
    for g in range(GROUPS):
        h = 1 - x
        swaps += [
            swap(wq_hbm.at[:, q_cols(h, g)], wa.at[g, f, x, c, :, pl.ds(0, qw)], 4 * g, 2 * g),
            swap(wk_hbm.at[:, k_cols(h, g)], wa.at[g, f, x, c, :, pl.ds(qw, kw)], 4 * g + 1, 2 * g),
            swap(wv_hbm.at[:, k_cols(h, g)], wv.at[g, f, x, c, pl.ds(0, rows)], 4 * g + 2, 2 * g + 1),
            swap(gain_tile, wv.at[g, f, x, c, pl.ds(rows, 16)], 4 * g + 3, 2 * g + 1),
        ]
    swaps.append(swap(hid_hbm, hid.at[1], 8, 6))
    swaps.append(swap(wo_hbm.at[:, oa_cols(1 - x)], woa.at[f, x, c], 9, 4))
    swaps.append(swap(wo_hbm.at[:, ob_cols(1 - x)], wob.at[f, x, c], 10, 5))
    for copy in swaps:
        copy.start()

    def swapped(ref, sem):
        swap(ref, ref, 0, sem).wait_recv()

    def ready(stage, xs):
        part = x if xs == 0 else 1 - x
        if stage < GROUPS:
            refs = ((wa.at[stage, f, part, c], 2 * stage),
                    (wv.at[stage, f, part, c, pl.ds(0, rows + 16 * xs)], 2 * stage + 1))
        else:
            refs = ((woa.at[f, part, c], 4), (wob.at[f, part, c], 5))
        for ref, sem in refs:
            if xs == 0:
                local(ref, ref, sem).wait()
            else:
                swapped(ref, sem)

    def stretch(number, cond=None):
        for plan, here, own in ((EDGE_PLAN, edge, 0), (MIDDLE_PLAN, middle, 1)):
            if plan[number]:
                def run(plan=plan, own=own):
                    for code in plan[number]:
                        if code < 100:
                            relay(code, own)
                        else:
                            stage, xs = (code - 100) // 2, (code - 100) % 2
                            ready(stage, xs)
                            kinds = ("a", "b") if stage < GROUPS else ("oa", "ob")
                            origin_ways(kinds, stage % GROUPS, x if xs == 0 else 1 - x, start,
                                        own == 1)
                pl.when(here if cond is None else here & cond)(run)

    def stretches(first, step, count):
        for number in range(count):
            stretch(first + number, step == number)

    def gain_row(zs):
        lane = lax.broadcasted_iota(jnp.int32, (1, LANES), 1)
        parts = []
        for col in range(2):
            for xs in range(2):
                low = wv[0, zs * 2 + col, xs, 0, rows:rows + 16, :].astype(jnp.float32)[0:1]
                high = wv[0, zs * 2 + col, xs, 1, rows:rows + 16, :].astype(jnp.float32)[0:1]
                parts.append(jnp.where(lane < rows, low, high))
        return jnp.concatenate(parts, axis=1)

    def normalize(t, zs, inv):
        cols = pl.ds(pl.multiple_of(zs * span, LANES), span)
        value = hid[t, :, cols].astype(jnp.float32) * inv * gain_row(zs)
        nrm[pl.ds(t * tokens, tokens), cols] = value.astype(jnp.bfloat16)

    def project(t, g, zs):
        cols = pl.ds(pl.multiple_of(zs * span, LANES), span)
        left = nrm[pl.ds(t * tokens, tokens), cols]
        fs = pl.ds(zs * 2, 2)
        weight = jnp.concatenate(
            [wa[g, fs].reshape(span, qw + kw), wv[g, fs, :, :, 0:rows, :].reshape(span, kw)], axis=1)
        acc[g, pl.ds(t * tokens, tokens), :] += jnp.dot(
            left, weight, preferred_element_type=jnp.float32)

    def attend(g, t):
        base = t * tokens
        span_rows = pl.ds(base, tokens)
        lane = lax.broadcasted_iota(jnp.int32, (tokens, LANES), 1)
        first = lane % HD < HD // 2
        left_head = lane < HD

        def turn(tile):
            turned = jnp.where(first, pltpu.roll(tile, LANES - HD // 2, 1),
                               pltpu.roll(tile, HD // 2, 1))
            return tile * cos_ref[...] + turned * sin_ref[...]

        key = turn(acc[g, span_rows, qw:qw + kw])
        value = acc[g, span_rows, qw + kw:qw + 2 * kw]
        key_other, value_other = pltpu.roll(key, HD, 1), pltpu.roll(value, HD, 1)
        for j in range(kw // HD):
            def low_high(tile, tile_other):
                low = tile if j == 0 else tile_other
                high = tile_other if j == 0 else tile
                zero = jnp.zeros_like(tile)
                return (jnp.where(left_head, low, zero).astype(jnp.bfloat16),
                        jnp.where(left_head, zero, high).astype(jnp.bfloat16))

            key_low, key_high = low_high(key, key_other)
            value_low, value_high = low_high(value, value_other)
            heads = qw // (kw // HD)
            query = []
            for p in range(heads // LANES):
                at = j * heads + p * LANES
                tile = turn(acc[g, span_rows, at:at + LANES])
                query.append(tile.astype(jnp.bfloat16) * jnp.bfloat16(HD ** -0.5))
            block = tokens // 2
            for b in range(2):
                seen = (b + 1) * block
                rows_q = slice(b * block, (b + 1) * block)
                stacked = jnp.concatenate([q[rows_q] for q in query], axis=0)
                keys = jnp.concatenate([key_low[:seen], key_high[:seen]], axis=0)
                values = jnp.concatenate([value_low[:seen], value_high[:seen]], axis=0)
                scores = lax.dot_general(stacked, keys, NT, preferred_element_type=jnp.float32)
                count = stacked.shape[0]
                at_row = lax.broadcasted_iota(jnp.int32, (count, seen), 0) % block + b * block
                at_col = lax.broadcasted_iota(jnp.int32, (count, seen), 1)
                open_ = at_row >= at_col
                probs = []
                for e in range(2):
                    part = jnp.where(open_, scores[:, e * seen:(e + 1) * seen], -1e30)
                    top = jnp.max(part, axis=-1, keepdims=True)
                    expo = jnp.exp(part - top)
                    total = jnp.sum(expo, axis=-1, keepdims=True)
                    probs.append((expo * (1.0 / total)).astype(jnp.bfloat16))
                mixed = jnp.dot(jnp.concatenate(probs, axis=1), values,
                                preferred_element_type=jnp.float32).astype(jnp.bfloat16)
                for p in range(heads // LANES):
                    at = g * qw + j * heads + p * LANES
                    ctx[pl.ds(base + b * block, block), at:at + LANES] = (
                        mixed[p * block:(p + 1) * block])

    def out_weight(s):
        fs = pl.ds(nearest(z, s) * 2, 2)
        return jnp.concatenate(
            [woa[fs].reshape(span, cut), wob[fs].reshape(span, half_out - cut)], axis=1)

    def share(s):
        return pltpu.make_async_remote_copy(
            src_ref=psend.at[s], dst_ref=precv.at[s], send_sem=psend_sem.at[s],
            recv_sem=precv_sem.at[s], device_id=partner, device_id_type=MESH)

    def out_other(s):
        part = lax.dot_general(ctx[tokens:2 * tokens, :], out_weight(s), NT,
                               preferred_element_type=jnp.float32)
        psend[s] = part.astype(jnp.bfloat16)
        share(s).start()

    def out_own(s):
        cols = pl.ds(pl.multiple_of(nearest(z, s) * span, LANES), span)
        part = lax.dot_general(ctx[0:tokens, :], out_weight(s), NT,
                               preferred_element_type=jnp.float32)
        own[s] = hid[0, :, cols].astype(jnp.float32) + part

    def close(s):
        share(s).wait_recv()
        cols = pl.ds(pl.multiple_of(nearest(z, s) * span, LANES), span)
        out_ref[:, cols] = (own[s] + precv[s].astype(jnp.float32)).astype(jnp.bfloat16)

    def own_first(i, carry):
        stretches(0, i, Z_LINE)
        sibling_arrived(("a", "b"), 0, i)
        normalize(0, nearest(z, i), inv_own)
        project(0, 0, nearest(z, i))
        return carry

    lax.fori_loop(0, Z_LINE, own_first, 0)
    local(cos_hbm, cos_ref, 7).wait()
    local(sin_hbm, sin_ref, 8).wait()
    stretch(4)
    attend(0, 0)
    stretch(5)
    swap(hid_hbm, hid.at[1], 8, 6).wait_recv()
    inv_other = inverse_rms(1)

    def other_first(i, carry):
        stretches(6, i, Z_LINE)
        normalize(1, i, inv_other)
        project(1, 0, i)
        return carry

    lax.fori_loop(0, Z_LINE, other_first, 0)
    stretch(10)
    attend(0, 1)

    def other_second(i, carry):
        stretches(11, i, Z_LINE)
        sibling_arrived(("a", "b"), 1, i)
        project(1, 1, nearest(z, i))
        return carry

    lax.fori_loop(0, Z_LINE, other_second, 0)
    stretch(15)
    attend(1, 1)
    stretch(16)
    sibling_arrived(("oa", "ob"), 0, 0)
    out_other(0)

    def own_second(i, carry):
        stretches(17, i, Z_LINE)
        project(0, 1, i)
        return carry

    lax.fori_loop(0, Z_LINE, own_second, 0)
    stretch(21)
    sibling_arrived(("oa", "ob"), 0, 1)
    out_other(1)
    stretch(22)
    attend(1, 0)

    def out_step(s, carry):
        for number in range(2):
            stretch(23 + 2 * number, s == number)
        out_own(s)
        for number in range(2):
            stretch(24 + 2 * number, s == number)
        sibling_arrived(("oa", "ob"), 0, s + 2)
        out_other(s + 2)
        return carry

    lax.fori_loop(0, 2, out_step, 0)
    for number in range(27, len(EDGE_PLAN)):
        stretch(number)

    def out_last(s, carry):
        out_own(s)
        return carry

    lax.fori_loop(2, Z_LINE, out_last, 0)

    for copy in swaps:
        copy.wait_send()
    for xs in range(2):
        for g in range(GROUPS):
            origin_ways(("a", "b"), g, xs, finish, middle)
        origin_ways(("oa", "ob"), 0, xs, finish, middle)

    def drain(k, carry):
        for kind, g in PIECES:
            sent(kind, g, k)
        return carry

    lax.fori_loop(0, Z_LINE, drain, 0)

    def close_step(s, carry):
        close(s)
        share(s).wait_send()
        return carry

    lax.fori_loop(0, Z_LINE, close_step, 0)


def fused(hidden, attn_gain, w_query, w_key, w_value, w_out):
    tokens, width = hidden.shape
    rows, width_query = w_query.shape
    width_kv = w_key.shape[1]
    fsdp = Z_LINE * 2
    qw, kw = width_query // 2 // GROUPS, width_kv // 2 // GROUPS
    half_out = width_query // 2
    span = width // Z_LINE
    cos_table, sin_table = lane_tables(tokens)
    kinds = 2 * GROUPS + 2
    dma = pltpu.SemaphoreType.DMA
    return pl.pallas_call(
        block_kernel,
        out_shape=jax.ShapeDtypeStruct((tokens, width), hidden.dtype),
        in_specs=[pl.BlockSpec(memory_space=pl.ANY)] * 8,
        out_specs=pl.BlockSpec(memory_space=pltpu.VMEM),
        scratch_shapes=[
            pltpu.VMEM((GROUPS, fsdp, 2, 2, rows, qw + kw), jnp.bfloat16),
            pltpu.VMEM((GROUPS, fsdp, 2, 2, rows + 16, kw), jnp.bfloat16),
            pltpu.VMEM((fsdp, 2, 2, rows, half_out - LANES), jnp.bfloat16),
            pltpu.VMEM((fsdp, 2, 2, rows, LANES), jnp.bfloat16),
            pltpu.VMEM((2, tokens, width), jnp.bfloat16),
            pltpu.VMEM((2 * tokens, width), jnp.bfloat16),
            pltpu.VMEM((GROUPS, 2 * tokens, qw + 2 * kw), jnp.float32),
            pltpu.VMEM((2 * tokens, half_out), jnp.bfloat16),
            pltpu.VMEM((tokens, LANES), jnp.float32),
            pltpu.VMEM((tokens, LANES), jnp.float32),
            pltpu.VMEM((Z_LINE, tokens, span), jnp.bfloat16),
            pltpu.VMEM((Z_LINE, tokens, span), jnp.bfloat16),
            pltpu.VMEM((Z_LINE, tokens, span), jnp.float32),
            pltpu.VMEM((1, rows), jnp.bfloat16),
            pltpu.VMEM((16, LANES), jnp.bfloat16),
            dma((kinds, 2, 4)),
            dma((kinds, fsdp, 4)),
            dma((kinds, fsdp)),
            dma((kinds, fsdp)),
            dma((11,)),
            dma((7,)),
            dma((10,)),
            dma((Z_LINE,)),
            dma((Z_LINE,)),
        ],
        compiler_params=pltpu.CompilerParams(
            collective_id=0, has_side_effects=True, vmem_limit_bytes=40 * 1024 * 1024),
        name="attention_block",
    )(*[pltpu.with_memory_space_constraint(value, pltpu.HBM) for value in (
        hidden, attn_gain[None, :], w_query, w_key, w_value, w_out.T,
        jnp.asarray(cos_table), jnp.asarray(sin_table))])


def fits(fsdp, rep, hidden, w_query, w_key, w_out):
    tokens, width = hidden.shape
    rows, width_query = w_query.shape
    return (
        rep == 4
        and fsdp == 2 * Z_LINE
        and 2 * rows == LANES
        and width == fsdp * rep * rows
        and w_out.shape == (width_query, rows)
        and w_key.shape[1] == 2 * GROUPS * LANES
        and width_query == 4 * w_key.shape[1]
        and tokens % LANES == 0
    )


def body(fsdp, rep, hidden, attn_gain, w_query, w_key, w_value, w_out):
    if fits(fsdp, rep, hidden, w_query, w_key, w_out):
        return fused(hidden, attn_gain, w_query, w_key, w_value, w_out)
    tokens = hidden.shape[0]
    head_dim = HD
    width_query = w_query.shape[1]
    width_kv = w_key.shape[1]
    kv_count = width_kv // head_dim
    group = width_query // width_kv
    x_float = hidden.astype(jnp.float32)
    inv_rms = lax.rsqrt(jnp.mean(x_float * x_float, axis=-1, keepdims=True) + norm_eps)
    width_rows = w_query.shape[0]
    packed = jnp.concatenate(
        [w_query, w_key, w_value, w_out.T, jnp.broadcast_to(attn_gain[:, None], (width_rows, 128))],
        axis=1,
    )
    packed = lax.all_gather(packed, ("fsdp", "rep"), axis=0, tiled=True)
    cut_key = width_query
    cut_value = cut_key + width_kv
    cut_out = cut_value + width_kv
    cut_gain = cut_out + w_out.shape[0]
    query_piece = packed[:, :cut_key]
    key_piece = packed[:, cut_key:cut_value]
    value_piece = packed[:, cut_value:cut_out]
    out_piece = packed[:, cut_out:cut_gain]
    gain_piece = packed[:, cut_gain]
    normed = (x_float * inv_rms * gain_piece.astype(jnp.float32)[None, :]).astype(jnp.bfloat16)
    queries = jnp.dot(normed, query_piece, preferred_element_type=jnp.float32)
    keys_raw = jnp.dot(normed, key_piece, preferred_element_type=jnp.float32)
    values_raw = jnp.dot(normed, value_piece, preferred_element_type=jnp.float32)
    cos_table, sin_table = rope_tables(tokens, head_dim)
    queries = queries.reshape(tokens, kv_count, group, head_dim)
    keys_raw = keys_raw.reshape(tokens, kv_count, head_dim)
    values_bf = values_raw.reshape(tokens, kv_count, head_dim).astype(jnp.bfloat16)
    rope_queries = rotate(queries, cos_table[:, None, None, :], sin_table[:, None, None, :]).astype(
        jnp.bfloat16
    )
    rope_keys = rotate(keys_raw, cos_table[:, None, :], sin_table[:, None, :]).astype(jnp.bfloat16)
    scores = jnp.einsum(
        "qkgd,skd->kgqs", rope_queries, rope_keys, preferred_element_type=jnp.float32
    ) * head_dim ** (-0.5)
    causal = jnp.arange(tokens)[:, None] >= jnp.arange(tokens)[None, :]
    scores = jnp.where(causal[None, None, :, :], scores, -1e30)
    top = jnp.max(scores, axis=-1, keepdims=True)
    expo = jnp.exp(scores - top)
    probs = (expo / jnp.sum(expo, axis=-1, keepdims=True)).astype(jnp.bfloat16)
    context = jnp.einsum("kgqs,skd->qkgd", probs, values_bf, preferred_element_type=jnp.float32)
    context = context.reshape(tokens, width_query).astype(jnp.bfloat16)
    branch = lax.dot_general(
        context, out_piece, (((1,), (1,)), ((), ())), preferred_element_type=jnp.float32
    )
    return (x_float + branch).astype(jnp.bfloat16)


def solution(mesh):
    placed = (
        P(("fsdp", "rep"), None),
        P(("fsdp", "rep")),
        P(("fsdp", "rep"), None),
        P(("fsdp", "rep"), None),
        P(("fsdp", "rep"), None),
        P(None, ("fsdp", "rep")),
    )
    return jax.shard_map(
        functools.partial(body, mesh.shape["fsdp"], mesh.shape["rep"]),
        mesh=mesh,
        in_specs=placed,
        out_specs=P(("fsdp", "rep"), None),
        check_vma=False,
    )
```

```python
import functools

import jax
import jax.numpy as jnp
import numpy as np
from jax import lax
from jax.experimental import pallas as pl
from jax.experimental.pallas import tpu as pltpu
from jax.sharding import PartitionSpec as P

HD = 64
LANES = 128
GROUPS = 2
Z_LINE = 4

rope_base = 500000.0
norm_eps = 1e-05

MESH = pl.DeviceIdType.MESH
NT = (((1,), (1,)), ((), ()))
TN = (((0,), (0,)), ((), ()))

BUFFERS = ("a", "b", "oa", "ob")
PIECES = (("a", 0), ("a", 1), ("b", 0), ("b", 1), ("oa", 0), ("ob", 0))
EDGE_PLAN = (
    (102, 100, 101, 103, 20, 1, 4, 28, 17, 104, 2, 3, 21, 9, 23, 22,),
    (25, 18, 12, 19, 6, 7, 5,),
    (10,),
    (),
    (),
    (),
    (),
    (11, 13,),
    (),
    (14, 27, 29, 105,),
    (31,),
    (30, 26, 15,),
    (),
    (),
    (),
    (),
    (),
    (33, 36, 44,),
    (),
    (41,),
    (),
    (),
    (),
    (34, 37, 45,),
    (42,),
    (),
    (35,),
    (46, 38,),
    (43,),
    (47,),
    (39,),
    (),
    (),
    (),
    (),
    (),
    (),
    (),
    (),
    (),
    (),
    (),
)
MIDDLE_PLAN = (
    (102, 100, 101, 103, 0, 16, 21, 2, 5, 28, 20, 29, 4, 3, 6, 24, 23, 8, 22,),
    (19, 18, 7, 10, 11, 27, 26, 31, 12, 13,),
    (),
    (),
    (),
    (30,),
    (104,),
    (),
    (),
    (14,),
    (105,),
    (),
    (15,),
    (),
    (),
    (32, 34,),
    (),
    (45, 37, 40,),
    (),
    (),
    (),
    (42, 36, 44, 35,),
    (46,),
    (),
    (43,),
    (),
    (38,),
    (),
    (),
    (),
    (),
    (39, 47,),
    (),
    (),
    (),
    (),
    (),
    (),
    (),
    (),
    (),
    (),
)


def rope_tables(tokens, head_dim):
    position = jnp.arange(tokens, dtype=jnp.float32)
    freq = rope_base ** (-(jnp.arange(head_dim // 2, dtype=jnp.float32) * 2.0) / head_dim)
    angle = position[:, None] * freq[None, :]
    cos_table = jnp.concatenate([jnp.cos(angle), jnp.cos(angle)], axis=-1)
    sin_table = jnp.concatenate([jnp.sin(angle), jnp.sin(angle)], axis=-1)
    return (cos_table, sin_table)


def rotate(tensor, cos_table, sin_table):
    half = tensor.shape[-1] // 2
    turned = jnp.concatenate([-tensor[..., half:], tensor[..., :half]], axis=-1)
    return tensor * cos_table + turned * sin_table


def lane_tables(tokens):
    lane = np.arange(LANES)
    freq = np.float64(rope_base) ** (-(lane % (HD // 2)) * 2.0 / HD)
    angle = np.arange(tokens)[:, None] * freq[None, :]
    sign = np.where(lane % HD < HD // 2, -1.0, 1.0)
    return np.cos(angle).astype(np.float32), (np.sin(angle) * sign).astype(np.float32)


def nearest(p, step):
    middle = jnp.where((p == 1) | (p == 2), 1, 0)
    high = step // 2
    low = step % 2
    low = low + middle * high * (1 - 2 * low)
    first = (1 - 2 * (p % 2)) * low
    return p + first + (2 - 4 * (p // 2)) * high


def block_kernel(
    hid_hbm, gain_hbm, wq_hbm, wk_hbm, wv_hbm, wo_hbm, cos_hbm, sin_hbm, own_out, other_out,
    wa, wv, woa, wob, hid, nrm, acc, ctx, cos_ref, sin_ref, psend, own, gain_in, gain_tile,
    send_sem, recv_sem, sib_sem, sibo_sem, xsend_sem, xrecv_sem, local_sem,
    psend_sem, precv_sem, own_sem,
):
    f, r = lax.axis_index("fsdp"), lax.axis_index("rep")
    z, y = f // 2, f % 2
    x, c = r // 2, r % 2
    tokens, width = hid.shape[1], hid.shape[2]
    rows = wa.shape[4]
    qw = wq_hbm.shape[1] // 2 // GROUPS
    kw = wk_hbm.shape[1] // 2 // GROUPS
    cut = woa.shape[4]
    half_out = cut + wob.shape[4]
    span = width // Z_LINE
    piece_cols = 4 * rows
    partner = (f, (1 - x) * 2 + c)
    sibling = (f, x * 2 + 1 - c)
    across = (z * 2 + 1 - y, r)
    low_half = z < Z_LINE // 2
    edge = (z == 0) | (z == Z_LINE - 1)
    middle = jnp.logical_not(edge)
    toward = jnp.where(low_half, 2, -2)
    outward = (f - toward, r)
    inward = (f + toward, r)
    mine = jnp.where(edge, 0, 1)

    def at_line(k):
        return jnp.where(low_half, k, Z_LINE - 1 - k)

    def view(kind, g, fs, which):
        if kind == "a":
            return wa.at[g, fs, :, which]
        if kind == "b":
            return wv.at[g, fs, :, which]
        if kind == "oa":
            return woa.at[fs, :, which]
        return wob.at[fs, :, which]

    def index(kind, g):
        return {"a": g, "b": GROUPS + g, "oa": 2 * GROUPS, "ob": 2 * GROUPS + 1}[kind]

    targets = {"outward": (0, outward), "inward": (1, inward), "across": (2, across),
               "sibling": (3, sibling)}

    def arrival(kind, k, fs, way):
        if way != "sibling":
            return recv_sem.at[k, fs]
        if kind in ("a", "b"):
            return sib_sem.at[k, fs // 2]
        return sibo_sem.at[k - 2 * GROUPS, fs]

    def remote(kind, g, fs, way):
        number, target = targets[way]
        k = index(kind, g)
        ref = view(kind, g, fs, c)
        return pltpu.make_async_remote_copy(
            src_ref=ref, dst_ref=ref, send_sem=send_sem.at[BUFFERS.index(kind), number],
            recv_sem=arrival(kind, k, fs, way), device_id=target, device_id_type=MESH)

    def origin(kind, g, xs, way):
        number, target = targets[way]
        k = index(kind, g)
        ref = view(kind, g, f, c).at[xs]
        return pltpu.make_async_remote_copy(
            src_ref=ref, dst_ref=ref, send_sem=send_sem.at[BUFFERS.index(kind), number],
            recv_sem=arrival(kind, k, f, way), device_id=target, device_id_type=MESH)

    def relay(piece, own):
        kind, g = PIECES[piece // 8]
        col, k = piece // 4 % 2, piece % 4
        main = kind in ("a", "oa")
        fs = at_line(k) * 2 + (y if col == 0 else 1 - y)
        remote(kind, g, fs, "across").wait_recv()
        if not (main and col == 1):
            if k >= own and own > 0:
                remote(kind, g, fs, "outward").start()
            if k <= own:
                remote(kind, g, fs, "inward").start()
            if main and col == 0:
                remote(kind, g, fs, "across").start()
        remote(kind, g, fs, "sibling").start()

    def sent(way, main_count, side_count):
        number, target = targets[way]
        for buffer, kind in enumerate(BUFFERS):
            count = pl.ds(0, main_count if kind in ("a", "oa") else side_count)
            ref = {"a": lambda: wa.at[:, count, :, c], "b": lambda: wv.at[:, count, :, c],
                   "oa": lambda: woa.at[count, :, c], "ob": lambda: wob.at[count, :, c]}[kind]()
            pltpu.make_async_remote_copy(
                src_ref=ref, dst_ref=ref, send_sem=send_sem.at[buffer, number],
                recv_sem=recv_sem.at[0, 0], device_id=target, device_id_type=MESH).wait_send()

    def origin_ways(kinds, g, xs, own):
        for kind in kinds:
            for way in targets:
                if way != "outward" or own > 0:
                    origin(kind, g, xs, way).start()

    def sibling_arrived(kinds, g, s):
        zs = nearest(z, s)
        both = pl.ds(zs * 2, 2)
        for kind in kinds:
            ref = view(kind, g, both, 1 - c)
            pltpu.make_async_remote_copy(
                src_ref=ref, dst_ref=ref, send_sem=send_sem.at[0, 3],
                recv_sem=sib_sem.at[index(kind, g), zs], device_id=sibling,
                device_id_type=MESH).wait_recv()

    def q_cols(h, g):
        return pl.ds(pl.multiple_of((h * GROUPS + g) * qw, LANES), qw)

    def k_cols(h, g):
        return pl.ds(pl.multiple_of((h * GROUPS + g) * kw, LANES), kw)

    def oa_cols(h):
        return pl.ds(pl.multiple_of(h * half_out, LANES), cut)

    def ob_cols(h):
        return pl.ds(pl.multiple_of(h * half_out + cut, LANES), half_out - cut)

    def local(src, dst, sem):
        return pltpu.make_async_copy(src, dst, local_sem.at[sem])

    local(gain_hbm, gain_in, 9).start()
    for g in range(GROUPS):
        local(wq_hbm.at[:, q_cols(x, g)], wa.at[g, f, x, c, :, pl.ds(0, qw)], 2 * g).start()
        local(wk_hbm.at[:, k_cols(x, g)], wa.at[g, f, x, c, :, pl.ds(qw, kw)], 2 * g).start()
        local(wv_hbm.at[:, k_cols(x, g)], wv.at[g, f, x, c, pl.ds(0, rows)], 2 * g + 1).start()
    local(wo_hbm.at[:, oa_cols(x)], woa.at[f, x, c], 4).start()
    local(wo_hbm.at[:, ob_cols(x)], wob.at[f, x, c], 5).start()
    local(hid_hbm, hid.at[0], 6).start()
    local(cos_hbm, cos_ref, 7).start()
    local(sin_hbm, sin_ref, 8).start()

    def inverse_rms(t):
        value = hid[t].astype(jnp.float32)
        return lax.rsqrt(jnp.mean(value * value, axis=-1, keepdims=True) + norm_eps)

    barrier = pltpu.get_barrier_semaphore()
    for target in (across, inward, partner, sibling):
        pl.semaphore_signal(barrier, inc=1, device_id=target, device_id_type=MESH)
    pl.when(middle)(lambda: pl.semaphore_signal(
        barrier, inc=1, device_id=outward, device_id_type=MESH))
    acc[...] = jnp.zeros_like(acc)
    local(gain_hbm, gain_in, 9).wait()
    gain = gain_in[...].astype(jnp.float32)
    gain = jnp.broadcast_to(jnp.concatenate([gain, gain], axis=1), (16, LANES))
    gain_tile[...] = gain.astype(jnp.bfloat16)
    for g in range(GROUPS):
        wv[g, f, x, c, rows:rows + 16, :] = gain.astype(jnp.bfloat16)
    local(hid_hbm, hid.at[0], 6).wait()
    inv_own = inverse_rms(0)
    pl.semaphore_wait(barrier, 4 + mine)

    def swap(src, dst, number, sem):
        return pltpu.make_async_remote_copy(
            src_ref=src, dst_ref=dst, send_sem=xsend_sem.at[number], recv_sem=xrecv_sem.at[sem],
            device_id=partner, device_id_type=MESH)

    swaps = []
    for g in range(GROUPS):
        h = 1 - x
        swaps += [
            swap(wq_hbm.at[:, q_cols(h, g)], wa.at[g, f, x, c, :, pl.ds(0, qw)], 0, 2 * g),
            swap(wk_hbm.at[:, k_cols(h, g)], wa.at[g, f, x, c, :, pl.ds(qw, kw)], 0, 2 * g),
            swap(wv_hbm.at[:, k_cols(h, g)], wv.at[g, f, x, c, pl.ds(0, rows)], 1, 2 * g + 1),
            swap(gain_tile, wv.at[g, f, x, c, pl.ds(rows, 16)], 1, 2 * g + 1),
        ]
    swaps.append(swap(hid_hbm, hid.at[1], 2, 6))
    swaps.append(swap(wo_hbm.at[:, oa_cols(1 - x)], woa.at[f, x, c], 3, 4))
    swaps.append(swap(wo_hbm.at[:, ob_cols(1 - x)], wob.at[f, x, c], 4, 5))
    for copy in swaps:
        copy.start()

    def swapped(ref, sem):
        swap(ref, ref, 0, sem).wait_recv()

    def ready(stage, xs):
        part = x if xs == 0 else 1 - x
        if stage < GROUPS:
            refs = ((wa.at[stage, f, part, c], 2 * stage),
                    (wv.at[stage, f, part, c, pl.ds(0, rows + 16 * xs)], 2 * stage + 1))
        else:
            refs = ((woa.at[f, part, c], 4), (wob.at[f, part, c], 5))
        for ref, sem in refs:
            if xs == 0:
                local(ref, ref, sem).wait()
            else:
                swapped(ref, sem)

    def stretch(number, cond=None):
        for plan, here, own in ((EDGE_PLAN, edge, 0), (MIDDLE_PLAN, middle, 1)):
            if plan[number]:
                def run(plan=plan, own=own):
                    for code in plan[number]:
                        if code < 100:
                            relay(code, own)
                        else:
                            stage, xs = (code - 100) // 2, (code - 100) % 2
                            ready(stage, xs)
                            kinds = ("a", "b") if stage < GROUPS else ("oa", "ob")
                            origin_ways(kinds, stage % GROUPS, x if xs == 0 else 1 - x, own)
                pl.when(here if cond is None else here & cond)(run)

    def stretches(first, step, count):
        for number in range(count):
            stretch(first + number, step == number)

    def gain_row(zs):
        lane = lax.broadcasted_iota(jnp.int32, (1, LANES), 1)
        parts = []
        for col in range(2):
            for xs in range(2):
                low = wv[0, zs * 2 + col, xs, 0, rows:rows + 16, :].astype(jnp.float32)[0:1]
                high = wv[0, zs * 2 + col, xs, 1, rows:rows + 16, :].astype(jnp.float32)[0:1]
                parts.append(jnp.where(lane < rows, low, high))
        return jnp.concatenate(parts, axis=1)

    def normalize(t, zs, inv):
        cols = pl.ds(pl.multiple_of(zs * span, LANES), span)
        value = hid[t, :, cols].astype(jnp.float32) * inv * gain_row(zs)
        nrm[pl.ds(t * tokens, tokens), cols] = value.astype(jnp.bfloat16)

    def project(t, g, zs):
        cols = pl.ds(pl.multiple_of(zs * span, LANES), span)
        left = nrm[pl.ds(t * tokens, tokens), cols]
        fs = pl.ds(zs * 2, 2)
        weight = jnp.concatenate(
            [wa[g, fs].reshape(span, qw + kw), wv[g, fs, :, :, 0:rows, :].reshape(span, kw)], axis=1)
        acc[g, pl.ds(t * tokens, tokens), :] += jnp.dot(
            left, weight, preferred_element_type=jnp.float32)

    def attend(g, t):
        base = t * tokens
        span_rows = pl.ds(base, tokens)
        lane = lax.broadcasted_iota(jnp.int32, (tokens, LANES), 1)
        first = lane % HD < HD // 2
        left_head = lane < HD

        def turn(tile):
            turned = jnp.where(first, pltpu.roll(tile, LANES - HD // 2, 1),
                               pltpu.roll(tile, HD // 2, 1))
            return tile * cos_ref[...] + turned * sin_ref[...]

        key = turn(acc[g, span_rows, qw:qw + kw])
        value = acc[g, span_rows, qw + kw:qw + 2 * kw]
        key_other, value_other = pltpu.roll(key, HD, 1), pltpu.roll(value, HD, 1)
        heads = qw // (kw // HD)
        block = tokens // 2
        wide = heads // LANES * block
        key_at = lax.broadcasted_iota(jnp.int32, (block, wide), 0)
        open_ = lax.broadcasted_iota(jnp.int32, (block, wide), 1) % block >= key_at
        for j in range(kw // HD):
            def low_high(tile, tile_other):
                low = tile if j == 0 else tile_other
                high = tile_other if j == 0 else tile
                zero = jnp.zeros_like(tile)
                return (jnp.where(left_head, low, zero).astype(jnp.bfloat16),
                        jnp.where(left_head, zero, high).astype(jnp.bfloat16))

            key_low, key_high = low_high(key, key_other)
            value_low, value_high = low_high(value, value_other)
            query = []
            for p in range(heads // LANES):
                at = j * heads + p * LANES
                tile = turn(acc[g, span_rows, at:at + LANES])
                query.append(tile.astype(jnp.bfloat16) * jnp.bfloat16(HD ** -0.5))
            for b in range(2):
                seen = (b + 1) * block
                stacked = jnp.concatenate([q[b * block:seen] for q in query], axis=0)
                keys = jnp.concatenate([key_low[:seen], key_high[:seen]], axis=0)
                values = jnp.concatenate([value_low[:seen], value_high[:seen]], axis=0)
                scores = lax.dot_general(keys, stacked, NT, preferred_element_type=jnp.float32)
                probs = []
                for e in range(2):
                    begin, end = e * seen, (e + 1) * seen
                    part = jnp.where(open_, scores[end - block:end], -1e30)
                    if b > 0:
                        part = jnp.concatenate([scores[begin:end - block], part], axis=0)
                    expo = jnp.exp(part - jnp.max(part, axis=0, keepdims=True))
                    total = jnp.sum(expo, axis=0, keepdims=True)
                    probs.append((expo * (1.0 / total)).astype(jnp.bfloat16))
                mixed = lax.dot_general(jnp.concatenate(probs, axis=0), values, TN,
                                        preferred_element_type=jnp.float32).astype(jnp.bfloat16)
                for p in range(heads // LANES):
                    at = g * qw + j * heads + p * LANES
                    ctx[pl.ds(base + b * block, block), at:at + LANES] = (
                        mixed[p * block:(p + 1) * block])

    def place(s, col):
        return nearest(z, s) * 2 + (y if col == 0 else 1 - y)

    def block_cols(fs):
        return pl.ds(pl.multiple_of(fs * piece_cols, LANES), piece_cols)

    def out_part(fs):
        weight = jnp.concatenate([woa[fs].reshape(piece_cols, cut),
                                  wob[fs].reshape(piece_cols, half_out - cut)], axis=1)
        return lax.dot_general(ctx[tokens:2 * tokens, :], weight, NT,
                               preferred_element_type=jnp.float32)

    def out_other(s, col):
        fs = place(s, col)
        for kind in ("oa", "ob"):
            ref = view(kind, 0, fs, 1 - c)
            pltpu.make_async_remote_copy(
                src_ref=ref, dst_ref=ref, send_sem=send_sem.at[0, 3],
                recv_sem=sibo_sem.at[index(kind, 0) - 2 * GROUPS, fs], device_id=sibling,
                device_id_type=MESH).wait_recv()
        psend[fs] = out_part(fs).astype(jnp.bfloat16)
        pltpu.make_async_remote_copy(
            src_ref=psend.at[fs], dst_ref=other_out.at[:, block_cols(fs)], send_sem=psend_sem,
            recv_sem=precv_sem, device_id=partner, device_id_type=MESH).start()

    def out_own(s):
        zs = nearest(z, s)
        both = pl.ds(zs * 2, 2)
        weight = jnp.concatenate([woa[both].reshape(span, cut),
                                  wob[both].reshape(span, half_out - cut)], axis=1)
        part = lax.dot_general(ctx[0:tokens, :], weight, NT, preferred_element_type=jnp.float32)
        cols = pl.ds(pl.multiple_of(zs * span, LANES), span)
        own[zs] = hid[0, :, cols].astype(jnp.float32) + part
        pltpu.make_async_copy(own.at[zs], own_out.at[:, cols], own_sem).start()

    def own_first(i, carry):
        stretches(0, i, Z_LINE)
        sibling_arrived(("a", "b"), 0, i)
        normalize(0, nearest(z, i), inv_own)
        project(0, 0, nearest(z, i))
        return carry

    lax.fori_loop(0, Z_LINE, own_first, 0)
    local(cos_hbm, cos_ref, 7).wait()
    local(sin_hbm, sin_ref, 8).wait()
    stretch(4)
    attend(0, 0)
    stretch(5)
    swap(hid_hbm, hid.at[1], 2, 6).wait_recv()
    inv_other = inverse_rms(1)

    def other_first(i, carry):
        stretches(6, i, Z_LINE)
        normalize(1, i, inv_other)
        project(1, 0, i)
        return carry

    lax.fori_loop(0, Z_LINE, other_first, 0)
    stretch(10)
    attend(0, 1)

    def other_second(i, carry):
        stretches(11, i, Z_LINE)
        sibling_arrived(("a", "b"), 1, i)
        project(1, 1, nearest(z, i))
        return carry

    lax.fori_loop(0, Z_LINE, other_second, 0)
    stretch(15)
    attend(1, 1)
    stretch(16)
    out_other(0, 0)
    stretch(17)
    out_other(0, 1)

    def own_second(i, carry):
        stretches(18, i, Z_LINE)
        project(0, 1, i)
        return carry

    lax.fori_loop(0, Z_LINE, own_second, 0)
    stretch(22)
    out_other(1, 0)
    stretch(23)
    out_other(1, 1)
    stretch(24)
    attend(1, 0)
    stretch(25)
    out_other(2, 0)
    stretch(26)
    out_own(0)
    stretch(27)
    out_other(2, 1)
    stretch(28)
    out_own(1)
    stretch(29)
    out_other(3, 0)
    stretch(30)
    out_own(2)
    stretch(31)
    out_other(3, 1)
    stretch(32)
    out_own(3)
    for number in range(33, len(EDGE_PLAN)):
        stretch(number)

    for number, ref in enumerate((wa.at[:, f, 0, c], wv.at[:, f, 0, c], hid.at[1],
                                  woa.at[f, 0, c], wob.at[f, 0, c])):
        swap(ref, ref, number, 0).wait_send()
    sent("sibling", 2 * Z_LINE, 2 * Z_LINE)
    sent("across", Z_LINE, 1)
    pl.when(edge)(lambda: sent("inward", 1, 2))

    @pl.when(middle)
    def _():
        sent("inward", 2, 4)
        sent("outward", 3, 6)

    pltpu.make_async_copy(own, own, own_sem).wait()
    everything = pltpu.make_async_remote_copy(
        src_ref=psend, dst_ref=psend, send_sem=psend_sem, recv_sem=precv_sem, device_id=partner,
        device_id_type=MESH)
    everything.wait_send()
    everything.wait_recv()


def fused(hidden, attn_gain, w_query, w_key, w_value, w_out):
    tokens, width = hidden.shape
    rows, width_query = w_query.shape
    width_kv = w_key.shape[1]
    fsdp = Z_LINE * 2
    qw, kw = width_query // 2 // GROUPS, width_kv // 2 // GROUPS
    half_out = width_query // 2
    span = width // Z_LINE
    cos_table, sin_table = lane_tables(tokens)
    kinds = 2 * GROUPS + 2
    dma = pltpu.SemaphoreType.DMA
    own, other = pl.pallas_call(
        block_kernel,
        out_shape=(jax.ShapeDtypeStruct((tokens, width), jnp.float32),
                   jax.ShapeDtypeStruct((tokens, width), jnp.bfloat16)),
        in_specs=[pl.BlockSpec(memory_space=pl.ANY)] * 8,
        out_specs=(pl.BlockSpec(memory_space=pl.ANY), pl.BlockSpec(memory_space=pl.ANY)),
        scratch_shapes=[
            pltpu.VMEM((GROUPS, fsdp, 2, 2, rows, qw + kw), jnp.bfloat16),
            pltpu.VMEM((GROUPS, fsdp, 2, 2, rows + 16, kw), jnp.bfloat16),
            pltpu.VMEM((fsdp, 2, 2, rows, half_out - LANES), jnp.bfloat16),
            pltpu.VMEM((fsdp, 2, 2, rows, LANES), jnp.bfloat16),
            pltpu.VMEM((2, tokens, width), jnp.bfloat16),
            pltpu.VMEM((2 * tokens, width), jnp.bfloat16),
            pltpu.VMEM((GROUPS, 2 * tokens, qw + 2 * kw), jnp.float32),
            pltpu.VMEM((2 * tokens, half_out), jnp.bfloat16),
            pltpu.VMEM((tokens, LANES), jnp.float32),
            pltpu.VMEM((tokens, LANES), jnp.float32),
            pltpu.VMEM((fsdp, tokens, 4 * rows), jnp.bfloat16),
            pltpu.VMEM((Z_LINE, tokens, span), jnp.float32),
            pltpu.VMEM((1, rows), jnp.bfloat16),
            pltpu.VMEM((16, LANES), jnp.bfloat16),
            dma((len(BUFFERS), 4)),
            dma((kinds, fsdp)),
            dma((2 * GROUPS, Z_LINE)),
            dma((2, fsdp)),
            dma((5,)),
            dma((7,)),
            dma((10,)),
            dma,
            dma,
            dma,
        ],
        compiler_params=pltpu.CompilerParams(
            collective_id=0, has_side_effects=True, vmem_limit_bytes=40 * 1024 * 1024),
        name="attention_block",
    )(*[pltpu.with_memory_space_constraint(value, pltpu.HBM) for value in (
        hidden, attn_gain[None, :], w_query, w_key, w_value, w_out.T,
        jnp.asarray(cos_table), jnp.asarray(sin_table))])
    return (own + other.astype(jnp.float32)).astype(hidden.dtype)


def fits(fsdp, rep, hidden, w_query, w_key, w_out):
    tokens, width = hidden.shape
    rows, width_query = w_query.shape
    return (
        rep == 4
        and fsdp == 2 * Z_LINE
        and 2 * rows == LANES
        and width == fsdp * rep * rows
        and w_out.shape == (width_query, rows)
        and w_key.shape[1] == 2 * GROUPS * LANES
        and width_query == 4 * w_key.shape[1]
        and tokens % LANES == 0
    )


def body(fsdp, rep, hidden, attn_gain, w_query, w_key, w_value, w_out):
    if fits(fsdp, rep, hidden, w_query, w_key, w_out):
        return fused(hidden, attn_gain, w_query, w_key, w_value, w_out)
    tokens = hidden.shape[0]
    head_dim = HD
    width_query = w_query.shape[1]
    width_kv = w_key.shape[1]
    kv_count = width_kv // head_dim
    group = width_query // width_kv
    x_float = hidden.astype(jnp.float32)
    inv_rms = lax.rsqrt(jnp.mean(x_float * x_float, axis=-1, keepdims=True) + norm_eps)
    width_rows = w_query.shape[0]
    packed = jnp.concatenate(
        [w_query, w_key, w_value, w_out.T, jnp.broadcast_to(attn_gain[:, None], (width_rows, 128))],
        axis=1,
    )
    packed = lax.all_gather(packed, ("fsdp", "rep"), axis=0, tiled=True)
    cut_key = width_query
    cut_value = cut_key + width_kv
    cut_out = cut_value + width_kv
    cut_gain = cut_out + w_out.shape[0]
    query_piece = packed[:, :cut_key]
    key_piece = packed[:, cut_key:cut_value]
    value_piece = packed[:, cut_value:cut_out]
    out_piece = packed[:, cut_out:cut_gain]
    gain_piece = packed[:, cut_gain]
    normed = (x_float * inv_rms * gain_piece.astype(jnp.float32)[None, :]).astype(jnp.bfloat16)
    queries = jnp.dot(normed, query_piece, preferred_element_type=jnp.float32)
    keys_raw = jnp.dot(normed, key_piece, preferred_element_type=jnp.float32)
    values_raw = jnp.dot(normed, value_piece, preferred_element_type=jnp.float32)
    cos_table, sin_table = rope_tables(tokens, head_dim)
    queries = queries.reshape(tokens, kv_count, group, head_dim)
    keys_raw = keys_raw.reshape(tokens, kv_count, head_dim)
    values_bf = values_raw.reshape(tokens, kv_count, head_dim).astype(jnp.bfloat16)
    rope_queries = rotate(queries, cos_table[:, None, None, :], sin_table[:, None, None, :]).astype(
        jnp.bfloat16
    )
    rope_keys = rotate(keys_raw, cos_table[:, None, :], sin_table[:, None, :]).astype(jnp.bfloat16)
    scores = jnp.einsum(
        "qkgd,skd->kgqs", rope_queries, rope_keys, preferred_element_type=jnp.float32
    ) * head_dim ** (-0.5)
    causal = jnp.arange(tokens)[:, None] >= jnp.arange(tokens)[None, :]
    scores = jnp.where(causal[None, None, :, :], scores, -1e30)
    top = jnp.max(scores, axis=-1, keepdims=True)
    expo = jnp.exp(scores - top)
    probs = (expo / jnp.sum(expo, axis=-1, keepdims=True)).astype(jnp.bfloat16)
    context = jnp.einsum("kgqs,skd->qkgd", probs, values_bf, preferred_element_type=jnp.float32)
    context = context.reshape(tokens, width_query).astype(jnp.bfloat16)
    branch = lax.dot_general(
        context, out_piece, (((1,), (1,)), ((), ())), preferred_element_type=jnp.float32
    )
    return (x_float + branch).astype(jnp.bfloat16)


def solution(mesh):
    placed = (
        P(("fsdp", "rep"), None),
        P(("fsdp", "rep")),
        P(("fsdp", "rep"), None),
        P(("fsdp", "rep"), None),
        P(("fsdp", "rep"), None),
        P(None, ("fsdp", "rep")),
    )
    return jax.shard_map(
        functools.partial(body, mesh.shape["fsdp"], mesh.shape["rep"]),
        mesh=mesh,
        in_specs=placed,
        out_specs=P(("fsdp", "rep"), None),
        check_vma=False,
    )
```

```python
import functools

import jax
import jax.numpy as jnp
import numpy as np
from jax import lax
from jax.experimental import pallas as pl
from jax.experimental.pallas import tpu as pltpu
from jax.sharding import PartitionSpec as P

HD = 64
LANES = 128
GROUPS = 2
Z_LINE = 4

rope_base = 500000.0
norm_eps = 1e-05

MESH = pl.DeviceIdType.MESH
NT = (((1,), (1,)), ((), ()))
TN = (((0,), (0,)), ((), ()))

BUFFERS = ("a", "b", "oa", "ob")
PIECES = (("a", 0), ("a", 1), ("b", 0), ("b", 1), ("oa", 0), ("ob", 0))
EDGE_PLAN = (
    (102, 100, 101, 103, 4, 1, 20, 25, 17,),
    (18, 104, 28, 12, 2, 21, 5, 3, 9, 6, 22, 19, 23,),
    (7, 11,),
    (),
    (),
    (10,),
    (13,),
    (29, 27, 15,),
    (),
    (105, 31,),
    (26,),
    (30, 14,),
    (),
    (),
    (),
    (),
    (),
    (33, 41, 36, 44,),
    (),
    (),
    (),
    (),
    (),
    (34, 42, 45,),
    (37,),
    (),
    (),
    (35, 43,),
    (38,),
    (46,),
    (47,),
    (39,),
    (),
    (),
    (),
    (),
    (),
    (),
    (),
    (),
    (),
    (),
)
MIDDLE_PLAN = (
    (100, 102, 101, 103, 5, 0, 18, 16, 2, 21, 20, 13, 24, 3, 19,),
    (4, 22, 8, 6, 23,),
    (11, 7, 28,),
    (10, 29, 27,),
    (31,),
    (),
    (15, 12, 26,),
    (30,),
    (),
    (104,),
    (14, 105,),
    (),
    (),
    (),
    (),
    (),
    (32,),
    (34, 40, 42,),
    (),
    (37,),
    (),
    (),
    (),
    (44, 45, 35, 43,),
    (36,),
    (),
    (),
    (),
    (46,),
    (38, 47, 39,),
    (),
    (),
    (),
    (),
    (),
    (),
    (),
    (),
    (),
    (),
    (),
    (),
)
FIRST_ORDER = ((0, 2, 1, 3), (1, 0, 3, 2))
SECOND_ORDER = ((1, 3, 0, 2), (3, 0, 2, 1))
OTHER_ORDER = (
    ((0, 0), (0, 1), (1, 0), (0, 2), (1, 1), (0, 3), (1, 2), (1, 3)),
    ((0, 1), (0, 0), (0, 2), (0, 3), (1, 0), (1, 1), (1, 3), (1, 2)),
)
OWN_ORDER = ((0, 1, 2, 3), (0, 1, 3, 2))


def rope_tables(tokens, head_dim):
    position = jnp.arange(tokens, dtype=jnp.float32)
    freq = rope_base ** (-(jnp.arange(head_dim // 2, dtype=jnp.float32) * 2.0) / head_dim)
    angle = position[:, None] * freq[None, :]
    cos_table = jnp.concatenate([jnp.cos(angle), jnp.cos(angle)], axis=-1)
    sin_table = jnp.concatenate([jnp.sin(angle), jnp.sin(angle)], axis=-1)
    return (cos_table, sin_table)


def rotate(tensor, cos_table, sin_table):
    half = tensor.shape[-1] // 2
    turned = jnp.concatenate([-tensor[..., half:], tensor[..., :half]], axis=-1)
    return tensor * cos_table + turned * sin_table


def lane_tables(tokens):
    lane = np.arange(LANES)
    freq = np.float64(rope_base) ** (-(lane % (HD // 2)) * 2.0 / HD)
    angle = np.arange(tokens)[:, None] * freq[None, :]
    sign = np.where(lane % HD < HD // 2, -1.0, 1.0)
    return np.cos(angle).astype(np.float32), (np.sin(angle) * sign).astype(np.float32)


def block_kernel(
    hid_hbm, gain_hbm, wq_hbm, wk_hbm, wv_hbm, wo_hbm, cos_hbm, sin_hbm, own_out, other_out,
    wa, wv, woa, wob, hid, nrm, acc, ctx, cos_ref, sin_ref, psend, own, gain_in, gain_tile,
    send_sem, recv_sem, sib_sem, sibo_sem, xsend_sem, xrecv_sem, local_sem,
    psend_sem, precv_sem, own_sem,
):
    f, r = lax.axis_index("fsdp"), lax.axis_index("rep")
    z, y = f // 2, f % 2
    x, c = r // 2, r % 2
    tokens, width = hid.shape[1], hid.shape[2]
    rows = wa.shape[4]
    qw = wq_hbm.shape[1] // 2 // GROUPS
    kw = wk_hbm.shape[1] // 2 // GROUPS
    cut = woa.shape[4]
    half_out = cut + wob.shape[4]
    span = width // Z_LINE
    piece_cols = 4 * rows
    partner = (f, (1 - x) * 2 + c)
    sibling = (f, x * 2 + 1 - c)
    across = (z * 2 + 1 - y, r)
    low_half = z < Z_LINE // 2
    edge = (z == 0) | (z == Z_LINE - 1)
    middle = jnp.logical_not(edge)
    toward = jnp.where(low_half, 2, -2)
    outward = (f - toward, r)
    inward = (f + toward, r)
    mine = jnp.where(edge, 0, 1)

    def at_line(k):
        return jnp.where(low_half, k, Z_LINE - 1 - k)

    def view(kind, g, fs, which):
        if kind == "a":
            return wa.at[g, fs, :, which]
        if kind == "b":
            return wv.at[g, fs, :, which]
        if kind == "oa":
            return woa.at[fs, :, which]
        return wob.at[fs, :, which]

    def index(kind, g):
        return {"a": g, "b": GROUPS + g, "oa": 2 * GROUPS, "ob": 2 * GROUPS + 1}[kind]

    targets = {"outward": (0, outward), "inward": (1, inward), "across": (2, across),
               "sibling": (3, sibling)}

    def picked(i, orders):
        k = sum(jnp.where(i == j, jnp.where(edge, e, m), 0)
                for j, (e, m) in enumerate(zip(*orders)))
        return at_line(k)

    def arrival(kind, k, fs, way):
        if way != "sibling":
            return recv_sem.at[k, fs]
        if kind in ("a", "b"):
            return sib_sem.at[k, fs // 2]
        return sibo_sem.at[k - 2 * GROUPS, fs]

    def remote(kind, g, fs, way):
        number, target = targets[way]
        k = index(kind, g)
        ref = view(kind, g, fs, c)
        return pltpu.make_async_remote_copy(
            src_ref=ref, dst_ref=ref, send_sem=send_sem.at[BUFFERS.index(kind), number],
            recv_sem=arrival(kind, k, fs, way), device_id=target, device_id_type=MESH)

    def origin(kind, g, xs, way):
        number, target = targets[way]
        k = index(kind, g)
        ref = view(kind, g, f, c).at[xs]
        return pltpu.make_async_remote_copy(
            src_ref=ref, dst_ref=ref, send_sem=send_sem.at[BUFFERS.index(kind), number],
            recv_sem=arrival(kind, k, f, way), device_id=target, device_id_type=MESH)

    def relay(piece, own):
        kind, g = PIECES[piece // 8]
        col, k = piece // 4 % 2, piece % 4
        main = kind in ("a", "oa")
        fs = at_line(k) * 2 + (y if col == 0 else 1 - y)
        remote(kind, g, fs, "across").wait_recv()
        if not (main and col == 1):
            if k >= own and own > 0:
                remote(kind, g, fs, "outward").start()
            if k <= own:
                remote(kind, g, fs, "inward").start()
            if main and col == 0:
                remote(kind, g, fs, "across").start()
        remote(kind, g, fs, "sibling").start()

    def sent(way, main_count, side_count):
        number, target = targets[way]
        for buffer, kind in enumerate(BUFFERS):
            count = pl.ds(0, main_count if kind in ("a", "oa") else side_count)
            ref = {"a": lambda: wa.at[:, count, :, c], "b": lambda: wv.at[:, count, :, c],
                   "oa": lambda: woa.at[count, :, c], "ob": lambda: wob.at[count, :, c]}[kind]()
            pltpu.make_async_remote_copy(
                src_ref=ref, dst_ref=ref, send_sem=send_sem.at[buffer, number],
                recv_sem=recv_sem.at[0, 0], device_id=target, device_id_type=MESH).wait_send()

    def origin_ways(kinds, g, xs, own):
        for kind in kinds:
            for way in targets:
                if way != "outward" or own > 0:
                    origin(kind, g, xs, way).start()

    def sibling_arrived(kinds, g, zs):
        both = pl.ds(zs * 2, 2)
        for kind in kinds:
            ref = view(kind, g, both, 1 - c)
            pltpu.make_async_remote_copy(
                src_ref=ref, dst_ref=ref, send_sem=send_sem.at[0, 3],
                recv_sem=sib_sem.at[index(kind, g), zs], device_id=sibling,
                device_id_type=MESH).wait_recv()

    def q_cols(h, g):
        return pl.ds(pl.multiple_of((h * GROUPS + g) * qw, LANES), qw)

    def k_cols(h, g):
        return pl.ds(pl.multiple_of((h * GROUPS + g) * kw, LANES), kw)

    def oa_cols(h):
        return pl.ds(pl.multiple_of(h * half_out, LANES), cut)

    def ob_cols(h):
        return pl.ds(pl.multiple_of(h * half_out + cut, LANES), half_out - cut)

    def local(src, dst, sem):
        return pltpu.make_async_copy(src, dst, local_sem.at[sem])

    local(gain_hbm, gain_in, 9).start()
    for g in range(GROUPS):
        local(wq_hbm.at[:, q_cols(x, g)], wa.at[g, f, x, c, :, pl.ds(0, qw)], 2 * g).start()
        local(wk_hbm.at[:, k_cols(x, g)], wa.at[g, f, x, c, :, pl.ds(qw, kw)], 2 * g).start()
        local(wv_hbm.at[:, k_cols(x, g)], wv.at[g, f, x, c, pl.ds(0, rows)], 2 * g + 1).start()
    local(wo_hbm.at[:, oa_cols(x)], woa.at[f, x, c], 4).start()
    local(wo_hbm.at[:, ob_cols(x)], wob.at[f, x, c], 5).start()
    local(hid_hbm, hid.at[0], 6).start()
    local(cos_hbm, cos_ref, 7).start()
    local(sin_hbm, sin_ref, 8).start()

    def inverse_rms(t):
        value = hid[t].astype(jnp.float32)
        return lax.rsqrt(jnp.mean(value * value, axis=-1, keepdims=True) + norm_eps)

    barrier = pltpu.get_barrier_semaphore()
    for target in (across, inward, partner, sibling):
        pl.semaphore_signal(barrier, inc=1, device_id=target, device_id_type=MESH)
    pl.when(middle)(lambda: pl.semaphore_signal(
        barrier, inc=1, device_id=outward, device_id_type=MESH))
    acc[...] = jnp.zeros_like(acc)
    local(gain_hbm, gain_in, 9).wait()
    gain = gain_in[...].astype(jnp.float32)
    gain = jnp.broadcast_to(jnp.concatenate([gain, gain], axis=1), (16, LANES))
    gain_tile[...] = gain.astype(jnp.bfloat16)
    for g in range(GROUPS):
        wv[g, f, x, c, rows:rows + 16, :] = gain.astype(jnp.bfloat16)
    local(hid_hbm, hid.at[0], 6).wait()
    inv_own = inverse_rms(0)
    pl.semaphore_wait(barrier, 4 + mine)

    def swap(src, dst, number, sem):
        return pltpu.make_async_remote_copy(
            src_ref=src, dst_ref=dst, send_sem=xsend_sem.at[number], recv_sem=xrecv_sem.at[sem],
            device_id=partner, device_id_type=MESH)

    swaps = []
    for g in range(GROUPS):
        h = 1 - x
        swaps += [
            swap(wq_hbm.at[:, q_cols(h, g)], wa.at[g, f, x, c, :, pl.ds(0, qw)], 0, 2 * g),
            swap(wk_hbm.at[:, k_cols(h, g)], wa.at[g, f, x, c, :, pl.ds(qw, kw)], 0, 2 * g),
            swap(wv_hbm.at[:, k_cols(h, g)], wv.at[g, f, x, c, pl.ds(0, rows)], 1, 2 * g + 1),
            swap(gain_tile, wv.at[g, f, x, c, pl.ds(rows, 16)], 1, 2 * g + 1),
        ]
    swaps.append(swap(hid_hbm, hid.at[1], 2, 6))
    swaps.append(swap(wo_hbm.at[:, oa_cols(1 - x)], woa.at[f, x, c], 3, 4))
    swaps.append(swap(wo_hbm.at[:, ob_cols(1 - x)], wob.at[f, x, c], 4, 5))
    for copy in swaps:
        copy.start()

    def swapped(ref, sem):
        swap(ref, ref, 0, sem).wait_recv()

    def ready(stage, xs):
        part = x if xs == 0 else 1 - x
        if stage < GROUPS:
            refs = ((wa.at[stage, f, part, c], 2 * stage),
                    (wv.at[stage, f, part, c, pl.ds(0, rows + 16 * xs)], 2 * stage + 1))
        else:
            refs = ((woa.at[f, part, c], 4), (wob.at[f, part, c], 5))
        for ref, sem in refs:
            if xs == 0:
                local(ref, ref, sem).wait()
            else:
                swapped(ref, sem)

    def stretch(number, cond=None):
        for plan, here, own in ((EDGE_PLAN, edge, 0), (MIDDLE_PLAN, middle, 1)):
            if plan[number]:
                def run(plan=plan, own=own):
                    for code in plan[number]:
                        if code < 100:
                            relay(code, own)
                        else:
                            stage, xs = (code - 100) // 2, (code - 100) % 2
                            ready(stage, xs)
                            kinds = ("a", "b") if stage < GROUPS else ("oa", "ob")
                            origin_ways(kinds, stage % GROUPS, x if xs == 0 else 1 - x, own)
                pl.when(here if cond is None else here & cond)(run)

    def stretches(first, step, count):
        for number in range(count):
            stretch(first + number, step == number)

    def gain_row(zs):
        lane = lax.broadcasted_iota(jnp.int32, (1, LANES), 1)
        parts = []
        for col in range(2):
            for xs in range(2):
                low = wv[0, zs * 2 + col, xs, 0, rows:rows + 16, :].astype(jnp.float32)[0:1]
                high = wv[0, zs * 2 + col, xs, 1, rows:rows + 16, :].astype(jnp.float32)[0:1]
                parts.append(jnp.where(lane < rows, low, high))
        return jnp.concatenate(parts, axis=1)

    def normalize(t, zs, inv):
        cols = pl.ds(pl.multiple_of(zs * span, LANES), span)
        value = hid[t, :, cols].astype(jnp.float32) * inv * gain_row(zs)
        nrm[pl.ds(t * tokens, tokens), cols] = value.astype(jnp.bfloat16)

    def project(t, g, zs):
        cols = pl.ds(pl.multiple_of(zs * span, LANES), span)
        left = nrm[pl.ds(t * tokens, tokens), cols]
        fs = pl.ds(zs * 2, 2)
        weight = jnp.concatenate(
            [wa[g, fs].reshape(span, qw + kw), wv[g, fs, :, :, 0:rows, :].reshape(span, kw)], axis=1)
        acc[g, pl.ds(t * tokens, tokens), :] += jnp.dot(
            left, weight, preferred_element_type=jnp.float32)

    def attend(g, t):
        base = t * tokens
        span_rows = pl.ds(base, tokens)
        lane = lax.broadcasted_iota(jnp.int32, (tokens, LANES), 1)
        first = lane % HD < HD // 2
        left_head = lane < HD

        def turn(tile):
            turned = jnp.where(first, pltpu.roll(tile, LANES - HD // 2, 1),
                               pltpu.roll(tile, HD // 2, 1))
            return tile * cos_ref[...] + turned * sin_ref[...]

        key = turn(acc[g, span_rows, qw:qw + kw])
        value = acc[g, span_rows, qw + kw:qw + 2 * kw]
        key_other, value_other = pltpu.roll(key, HD, 1), pltpu.roll(value, HD, 1)
        heads = qw // (kw // HD)
        block = tokens // 2
        wide = heads // LANES * block
        key_at = lax.broadcasted_iota(jnp.int32, (block, wide), 0)
        open_ = lax.broadcasted_iota(jnp.int32, (block, wide), 1) % block >= key_at
        for j in range(kw // HD):
            def low_high(tile, tile_other):
                low = tile if j == 0 else tile_other
                high = tile_other if j == 0 else tile
                zero = jnp.zeros_like(tile)
                return (jnp.where(left_head, low, zero).astype(jnp.bfloat16),
                        jnp.where(left_head, zero, high).astype(jnp.bfloat16))

            key_low, key_high = low_high(key, key_other)
            value_low, value_high = low_high(value, value_other)
            query = []
            for p in range(heads // LANES):
                at = j * heads + p * LANES
                tile = turn(acc[g, span_rows, at:at + LANES])
                query.append(tile.astype(jnp.bfloat16) * jnp.bfloat16(HD ** -0.5))
            for b in range(2):
                seen = (b + 1) * block
                stacked = jnp.concatenate([q[b * block:seen] for q in query], axis=0)
                keys = jnp.concatenate([key_low[:seen], key_high[:seen]], axis=0)
                values = jnp.concatenate([value_low[:seen], value_high[:seen]], axis=0)
                scores = lax.dot_general(keys, stacked, NT, preferred_element_type=jnp.float32)
                probs = []
                for e in range(2):
                    begin, end = e * seen, (e + 1) * seen
                    part = jnp.where(open_, scores[end - block:end], -1e30)
                    if b > 0:
                        part = jnp.concatenate([scores[begin:end - block], part], axis=0)
                    expo = jnp.exp(part - jnp.max(part, axis=0, keepdims=True))
                    total = jnp.sum(expo, axis=0, keepdims=True)
                    probs.append((expo * (1.0 / total)).astype(jnp.bfloat16))
                mixed = lax.dot_general(jnp.concatenate(probs, axis=0), values, TN,
                                        preferred_element_type=jnp.float32).astype(jnp.bfloat16)
                for p in range(heads // LANES):
                    at = g * qw + j * heads + p * LANES
                    ctx[pl.ds(base + b * block, block), at:at + LANES] = (
                        mixed[p * block:(p + 1) * block])

    def place(n):
        col, k = (jnp.where(edge, OTHER_ORDER[0][n][which], OTHER_ORDER[1][n][which])
                  for which in range(2))
        return at_line(k) * 2 + jnp.where(col == 0, y, 1 - y)

    def block_cols(fs):
        return pl.ds(pl.multiple_of(fs * piece_cols, LANES), piece_cols)

    def out_part(fs):
        weight = jnp.concatenate([woa[fs].reshape(piece_cols, cut),
                                  wob[fs].reshape(piece_cols, half_out - cut)], axis=1)
        return lax.dot_general(ctx[tokens:2 * tokens, :], weight, NT,
                               preferred_element_type=jnp.float32)

    def out_other(n):
        fs = place(n)
        for kind in ("oa", "ob"):
            ref = view(kind, 0, fs, 1 - c)
            pltpu.make_async_remote_copy(
                src_ref=ref, dst_ref=ref, send_sem=send_sem.at[0, 3],
                recv_sem=sibo_sem.at[index(kind, 0) - 2 * GROUPS, fs], device_id=sibling,
                device_id_type=MESH).wait_recv()
        psend[fs] = out_part(fs).astype(jnp.bfloat16)
        pltpu.make_async_remote_copy(
            src_ref=psend.at[fs], dst_ref=other_out.at[:, block_cols(fs)], send_sem=psend_sem,
            recv_sem=precv_sem, device_id=partner, device_id_type=MESH).start()

    def out_own(n):
        zs = picked(n, OWN_ORDER)
        both = pl.ds(zs * 2, 2)
        weight = jnp.concatenate([woa[both].reshape(span, cut),
                                  wob[both].reshape(span, half_out - cut)], axis=1)
        part = lax.dot_general(ctx[0:tokens, :], weight, NT, preferred_element_type=jnp.float32)
        cols = pl.ds(pl.multiple_of(zs * span, LANES), span)
        own[zs] = hid[0, :, cols].astype(jnp.float32) + part
        pltpu.make_async_copy(own.at[zs], own_out.at[:, cols], own_sem).start()

    def own_first(i, carry):
        stretches(0, i, Z_LINE)
        zs = picked(i, FIRST_ORDER)
        sibling_arrived(("a", "b"), 0, zs)
        normalize(0, zs, inv_own)
        project(0, 0, zs)
        return carry

    lax.fori_loop(0, Z_LINE, own_first, 0)
    local(cos_hbm, cos_ref, 7).wait()
    local(sin_hbm, sin_ref, 8).wait()
    stretch(4)
    attend(0, 0)
    stretch(5)
    swap(hid_hbm, hid.at[1], 2, 6).wait_recv()
    inv_other = inverse_rms(1)

    def other_first(i, carry):
        stretches(6, i, Z_LINE)
        normalize(1, i, inv_other)
        project(1, 0, i)
        return carry

    lax.fori_loop(0, Z_LINE, other_first, 0)
    stretch(10)
    attend(0, 1)

    def other_second(i, carry):
        stretches(11, i, Z_LINE)
        zs = picked(i, SECOND_ORDER)
        sibling_arrived(("a", "b"), 1, zs)
        project(1, 1, zs)
        return carry

    lax.fori_loop(0, Z_LINE, other_second, 0)
    stretch(15)
    attend(1, 1)
    stretch(16)
    out_other(0)
    stretch(17)
    out_other(1)

    def own_second(i, carry):
        stretches(18, i, Z_LINE)
        project(0, 1, i)
        return carry

    lax.fori_loop(0, Z_LINE, own_second, 0)
    stretch(22)
    out_other(2)
    stretch(23)
    out_other(3)
    stretch(24)
    attend(1, 0)
    stretch(25)
    out_other(4)
    stretch(26)
    out_own(0)
    stretch(27)
    out_other(5)
    stretch(28)
    out_own(1)
    stretch(29)
    out_other(6)
    stretch(30)
    out_own(2)
    stretch(31)
    out_other(7)
    stretch(32)
    out_own(3)
    for number in range(33, len(EDGE_PLAN)):
        stretch(number)

    for number, ref in enumerate((wa.at[:, f, 0, c], wv.at[:, f, 0, c], hid.at[1],
                                  woa.at[f, 0, c], wob.at[f, 0, c])):
        swap(ref, ref, number, 0).wait_send()
    sent("sibling", 2 * Z_LINE, 2 * Z_LINE)
    sent("across", Z_LINE, 1)
    pl.when(edge)(lambda: sent("inward", 1, 2))

    @pl.when(middle)
    def _():
        sent("inward", 2, 4)
        sent("outward", 3, 6)

    pltpu.make_async_copy(own, own, own_sem).wait()
    everything = pltpu.make_async_remote_copy(
        src_ref=psend, dst_ref=psend, send_sem=psend_sem, recv_sem=precv_sem, device_id=partner,
        device_id_type=MESH)
    everything.wait_send()
    everything.wait_recv()


def fused(hidden, attn_gain, w_query, w_key, w_value, w_out):
    tokens, width = hidden.shape
    rows, width_query = w_query.shape
    width_kv = w_key.shape[1]
    fsdp = Z_LINE * 2
    qw, kw = width_query // 2 // GROUPS, width_kv // 2 // GROUPS
    half_out = width_query // 2
    span = width // Z_LINE
    cos_table, sin_table = lane_tables(tokens)
    kinds = 2 * GROUPS + 2
    dma = pltpu.SemaphoreType.DMA
    own, other = pl.pallas_call(
        block_kernel,
        out_shape=(jax.ShapeDtypeStruct((tokens, width), jnp.float32),
                   jax.ShapeDtypeStruct((tokens, width), jnp.bfloat16)),
        in_specs=[pl.BlockSpec(memory_space=pl.ANY)] * 8,
        out_specs=(pl.BlockSpec(memory_space=pl.ANY), pl.BlockSpec(memory_space=pl.ANY)),
        scratch_shapes=[
            pltpu.VMEM((GROUPS, fsdp, 2, 2, rows, qw + kw), jnp.bfloat16),
            pltpu.VMEM((GROUPS, fsdp, 2, 2, rows + 16, kw), jnp.bfloat16),
            pltpu.VMEM((fsdp, 2, 2, rows, half_out - LANES), jnp.bfloat16),
            pltpu.VMEM((fsdp, 2, 2, rows, LANES), jnp.bfloat16),
            pltpu.VMEM((2, tokens, width), jnp.bfloat16),
            pltpu.VMEM((2 * tokens, width), jnp.bfloat16),
            pltpu.VMEM((GROUPS, 2 * tokens, qw + 2 * kw), jnp.float32),
            pltpu.VMEM((2 * tokens, half_out), jnp.bfloat16),
            pltpu.VMEM((tokens, LANES), jnp.float32),
            pltpu.VMEM((tokens, LANES), jnp.float32),
            pltpu.VMEM((fsdp, tokens, 4 * rows), jnp.bfloat16),
            pltpu.VMEM((Z_LINE, tokens, span), jnp.float32),
            pltpu.VMEM((1, rows), jnp.bfloat16),
            pltpu.VMEM((16, LANES), jnp.bfloat16),
            dma((len(BUFFERS), 4)),
            dma((kinds, fsdp)),
            dma((2 * GROUPS, Z_LINE)),
            dma((2, fsdp)),
            dma((5,)),
            dma((7,)),
            dma((10,)),
            dma,
            dma,
            dma,
        ],
        compiler_params=pltpu.CompilerParams(
            collective_id=0, has_side_effects=True, vmem_limit_bytes=40 * 1024 * 1024),
        name="attention_block",
    )(*[pltpu.with_memory_space_constraint(value, pltpu.HBM) for value in (
        hidden, attn_gain[None, :], w_query, w_key, w_value, w_out.T,
        jnp.asarray(cos_table), jnp.asarray(sin_table))])
    return (own + other.astype(jnp.float32)).astype(hidden.dtype)


def fits(fsdp, rep, hidden, w_query, w_key, w_out):
    tokens, width = hidden.shape
    rows, width_query = w_query.shape
    return (
        rep == 4
        and fsdp == 2 * Z_LINE
        and 2 * rows == LANES
        and width == fsdp * rep * rows
        and w_out.shape == (width_query, rows)
        and w_key.shape[1] == 2 * GROUPS * LANES
        and width_query == 4 * w_key.shape[1]
        and tokens % LANES == 0
    )


def body(fsdp, rep, hidden, attn_gain, w_query, w_key, w_value, w_out):
    if fits(fsdp, rep, hidden, w_query, w_key, w_out):
        return fused(hidden, attn_gain, w_query, w_key, w_value, w_out)
    tokens = hidden.shape[0]
    head_dim = HD
    width_query = w_query.shape[1]
    width_kv = w_key.shape[1]
    kv_count = width_kv // head_dim
    group = width_query // width_kv
    x_float = hidden.astype(jnp.float32)
    inv_rms = lax.rsqrt(jnp.mean(x_float * x_float, axis=-1, keepdims=True) + norm_eps)
    width_rows = w_query.shape[0]
    packed = jnp.concatenate(
        [w_query, w_key, w_value, w_out.T, jnp.broadcast_to(attn_gain[:, None], (width_rows, 128))],
        axis=1,
    )
    packed = lax.all_gather(packed, ("fsdp", "rep"), axis=0, tiled=True)
    cut_key = width_query
    cut_value = cut_key + width_kv
    cut_out = cut_value + width_kv
    cut_gain = cut_out + w_out.shape[0]
    query_piece = packed[:, :cut_key]
    key_piece = packed[:, cut_key:cut_value]
    value_piece = packed[:, cut_value:cut_out]
    out_piece = packed[:, cut_out:cut_gain]
    gain_piece = packed[:, cut_gain]
    normed = (x_float * inv_rms * gain_piece.astype(jnp.float32)[None, :]).astype(jnp.bfloat16)
    queries = jnp.dot(normed, query_piece, preferred_element_type=jnp.float32)
    keys_raw = jnp.dot(normed, key_piece, preferred_element_type=jnp.float32)
    values_raw = jnp.dot(normed, value_piece, preferred_element_type=jnp.float32)
    cos_table, sin_table = rope_tables(tokens, head_dim)
    queries = queries.reshape(tokens, kv_count, group, head_dim)
    keys_raw = keys_raw.reshape(tokens, kv_count, head_dim)
    values_bf = values_raw.reshape(tokens, kv_count, head_dim).astype(jnp.bfloat16)
    rope_queries = rotate(queries, cos_table[:, None, None, :], sin_table[:, None, None, :]).astype(
        jnp.bfloat16
    )
    rope_keys = rotate(keys_raw, cos_table[:, None, :], sin_table[:, None, :]).astype(jnp.bfloat16)
    scores = jnp.einsum(
        "qkgd,skd->kgqs", rope_queries, rope_keys, preferred_element_type=jnp.float32
    ) * head_dim ** (-0.5)
    causal = jnp.arange(tokens)[:, None] >= jnp.arange(tokens)[None, :]
    scores = jnp.where(causal[None, None, :, :], scores, -1e30)
    top = jnp.max(scores, axis=-1, keepdims=True)
    expo = jnp.exp(scores - top)
    probs = (expo / jnp.sum(expo, axis=-1, keepdims=True)).astype(jnp.bfloat16)
    context = jnp.einsum("kgqs,skd->qkgd", probs, values_bf, preferred_element_type=jnp.float32)
    context = context.reshape(tokens, width_query).astype(jnp.bfloat16)
    branch = lax.dot_general(
        context, out_piece, (((1,), (1,)), ((), ())), preferred_element_type=jnp.float32
    )
    return (x_float + branch).astype(jnp.bfloat16)


def solution(mesh):
    placed = (
        P(("fsdp", "rep"), None),
        P(("fsdp", "rep")),
        P(("fsdp", "rep"), None),
        P(("fsdp", "rep"), None),
        P(("fsdp", "rep"), None),
        P(None, ("fsdp", "rep")),
    )
    return jax.shard_map(
        functools.partial(body, mesh.shape["fsdp"], mesh.shape["rep"]),
        mesh=mesh,
        in_specs=placed,
        out_specs=P(("fsdp", "rep"), None),
        check_vma=False,
    )
```

```python
import functools

import jax
import jax.numpy as jnp
import numpy as np
from jax import lax
from jax.experimental import pallas as pl
from jax.experimental.pallas import tpu as pltpu
from jax.sharding import PartitionSpec as P

HD = 64
LANES = 128
GROUPS = 2
Z_LINE = 4

rope_base = 500000.0
norm_eps = 1e-05

MESH = pl.DeviceIdType.MESH
NT = (((1,), (1,)), ((), ()))
TN = (((0,), (0,)), ((), ()))

BUFFERS = ("a", "b", "oa", "ob")
PIECES = (("a", 0), ("a", 1), ("b", 0), ("b", 1), ("oa", 0), ("ob", 0))
EDGE_PLAN = (
    (100, 102, 101, 103, 1, 17, 20, 4, 28, 25, 18, 9, 5, 21, 12, 2,),
    (3, 13, 22, 19, 23, 104, 6, 7, 10,),
    (),
    (),
    (),
    (11,),
    (),
    (29,),
    (),
    (),
    (),
    (105, 14, 26,),
    (30, 15, 27,),
    (31,),
    (),
    (),
    (36,),
    (44, 33,),
    (),
    (),
    (41,),
    (),
    (),
    (34, 42,),
    (45, 37,),
    (),
    (),
    (35, 43,),
    (38, 47,),
    (46,),
    (),
    (39,),
    (),
    (),
    (),
    (),
    (),
    (),
    (),
    (),
    (),
    (),
)
MIDDLE_PLAN = (
    (100, 102, 101, 103, 0, 18, 21, 5, 2, 16, 20, 3, 8, 4, 13,),
    (22, 24, 19, 23, 28, 10, 11, 29, 27, 6, 26,),
    (7, 31,),
    (30, 104,),
    (),
    (12,),
    (),
    (),
    (14,),
    (),
    (105, 15,),
    (),
    (),
    (),
    (),
    (34,),
    (),
    (42, 32, 37,),
    (45,),
    (40,),
    (),
    (44,),
    (),
    (38,),
    (35,),
    (43,),
    (47, 46,),
    (36, 39,),
    (),
    (),
    (),
    (),
    (),
    (),
    (),
    (),
    (),
    (),
    (),
    (),
    (),
    (),
)
FIRST_ORDER = ((1, 0, 2, 3), (0, 1, 2, 3))
SECOND_ORDER = ((1, 0, 2, 3), (0, 2, 1, 3))
OTHER_ORDER = (
    ((0, 0), (1, 0), (0, 1), (0, 2), (1, 1), (0, 3), (1, 2), (1, 3)),
    ((0, 1), (0, 2), (1, 1), (0, 0), (0, 3), (1, 2), (1, 0), (1, 3)),
)
OWN_ORDER = ((0, 1, 2, 3), (1, 2, 0, 3))


def rope_tables(tokens, head_dim):
    position = jnp.arange(tokens, dtype=jnp.float32)
    freq = rope_base ** (-(jnp.arange(head_dim // 2, dtype=jnp.float32) * 2.0) / head_dim)
    angle = position[:, None] * freq[None, :]
    cos_table = jnp.concatenate([jnp.cos(angle), jnp.cos(angle)], axis=-1)
    sin_table = jnp.concatenate([jnp.sin(angle), jnp.sin(angle)], axis=-1)
    return (cos_table, sin_table)


def rotate(tensor, cos_table, sin_table):
    half = tensor.shape[-1] // 2
    turned = jnp.concatenate([-tensor[..., half:], tensor[..., :half]], axis=-1)
    return tensor * cos_table + turned * sin_table


def lane_tables(tokens):
    lane = np.arange(LANES)
    freq = np.float64(rope_base) ** (-(lane % (HD // 2)) * 2.0 / HD)
    angle = np.arange(tokens)[:, None] * freq[None, :]
    sign = np.where(lane % HD < HD // 2, -1.0, 1.0)
    return np.cos(angle).astype(np.float32), (np.sin(angle) * sign).astype(np.float32)


def block_kernel(
    hid_hbm, gain_hbm, wq_hbm, wk_hbm, wv_hbm, wo_hbm, cos_hbm, sin_hbm, own_out, other_out,
    wa, wv, woa, wob, hid, nrm, acc, ctx, cos_ref, sin_ref, psend, own, gain_in, gain_tile,
    send_sem, recv_sem, sib_sem, sibo_sem, xsend_sem, xrecv_sem, local_sem,
    psend_sem, precv_sem, own_sem,
):
    f, r = lax.axis_index("fsdp"), lax.axis_index("rep")
    z, y = f // 2, f % 2
    x, c = r // 2, r % 2
    tokens, width = hid.shape[1], hid.shape[2]
    rows = wa.shape[4]
    qw = wq_hbm.shape[1] // 2 // GROUPS
    kw = wk_hbm.shape[1] // 2 // GROUPS
    cut = woa.shape[4]
    half_out = cut + wob.shape[4]
    span = width // Z_LINE
    piece_cols = 4 * rows
    partner = (f, (1 - x) * 2 + c)
    sibling = (f, x * 2 + 1 - c)
    across = (z * 2 + 1 - y, r)
    low_half = z < Z_LINE // 2
    edge = (z == 0) | (z == Z_LINE - 1)
    middle = jnp.logical_not(edge)
    toward = jnp.where(low_half, 2, -2)
    outward = (f - toward, r)
    inward = (f + toward, r)
    mine = jnp.where(edge, 0, 1)

    def at_line(k):
        return jnp.where(low_half, k, Z_LINE - 1 - k)

    def view(kind, g, fs, which):
        if kind == "a":
            return wa.at[g, fs, :, which]
        if kind == "b":
            return wv.at[g, fs, :, which]
        if kind == "oa":
            return woa.at[fs, :, which]
        return wob.at[fs, :, which]

    def index(kind, g):
        return {"a": g, "b": GROUPS + g, "oa": 2 * GROUPS, "ob": 2 * GROUPS + 1}[kind]

    targets = {"outward": (0, outward), "inward": (1, inward), "across": (2, across),
               "sibling": (3, sibling)}

    def picked(i, orders):
        k = sum(jnp.where(i == j, jnp.where(edge, e, m), 0)
                for j, (e, m) in enumerate(zip(*orders)))
        return at_line(k)

    def arrival(kind, k, fs, way):
        if way != "sibling":
            return recv_sem.at[k, fs]
        if kind in ("a", "b"):
            return sib_sem.at[k, fs // 2]
        return sibo_sem.at[k - 2 * GROUPS, fs]

    def remote(kind, g, fs, way):
        number, target = targets[way]
        k = index(kind, g)
        ref = view(kind, g, fs, c)
        return pltpu.make_async_remote_copy(
            src_ref=ref, dst_ref=ref, send_sem=send_sem.at[BUFFERS.index(kind), number],
            recv_sem=arrival(kind, k, fs, way), device_id=target, device_id_type=MESH)

    def origin(kind, g, xs, way):
        number, target = targets[way]
        k = index(kind, g)
        ref = view(kind, g, f, c).at[xs]
        return pltpu.make_async_remote_copy(
            src_ref=ref, dst_ref=ref, send_sem=send_sem.at[BUFFERS.index(kind), number],
            recv_sem=arrival(kind, k, f, way), device_id=target, device_id_type=MESH)

    def relay(piece, own):
        kind, g = PIECES[piece // 8]
        col, k = piece // 4 % 2, piece % 4
        main = kind in ("a", "oa")
        fs = at_line(k) * 2 + (y if col == 0 else 1 - y)
        remote(kind, g, fs, "across").wait_recv()
        if not (main and col == 1):
            if k >= own and own > 0:
                remote(kind, g, fs, "outward").start()
            if k <= own:
                remote(kind, g, fs, "inward").start()
            if main and col == 0:
                remote(kind, g, fs, "across").start()
        remote(kind, g, fs, "sibling").start()

    def sent(way, main_count, side_count):
        number, target = targets[way]
        for buffer, kind in enumerate(BUFFERS):
            count = pl.ds(0, main_count if kind in ("a", "oa") else side_count)
            ref = {"a": lambda: wa.at[:, count, :, c], "b": lambda: wv.at[:, count, :, c],
                   "oa": lambda: woa.at[count, :, c], "ob": lambda: wob.at[count, :, c]}[kind]()
            pltpu.make_async_remote_copy(
                src_ref=ref, dst_ref=ref, send_sem=send_sem.at[buffer, number],
                recv_sem=recv_sem.at[0, 0], device_id=target, device_id_type=MESH).wait_send()

    def origin_ways(kinds, g, xs, own):
        for kind in kinds:
            for way in targets:
                if way != "outward" or own > 0:
                    origin(kind, g, xs, way).start()

    def sibling_arrived(kinds, g, zs):
        both = pl.ds(zs * 2, 2)
        for kind in kinds:
            ref = view(kind, g, both, 1 - c)
            pltpu.make_async_remote_copy(
                src_ref=ref, dst_ref=ref, send_sem=send_sem.at[0, 3],
                recv_sem=sib_sem.at[index(kind, g), zs], device_id=sibling,
                device_id_type=MESH).wait_recv()

    def q_cols(h, g):
        return pl.ds(pl.multiple_of((h * GROUPS + g) * qw, LANES), qw)

    def k_cols(h, g):
        return pl.ds(pl.multiple_of((h * GROUPS + g) * kw, LANES), kw)

    def oa_cols(h):
        return pl.ds(pl.multiple_of(h * half_out, LANES), cut)

    def ob_cols(h):
        return pl.ds(pl.multiple_of(h * half_out + cut, LANES), half_out - cut)

    def local(src, dst, sem):
        return pltpu.make_async_copy(src, dst, local_sem.at[sem])

    local(gain_hbm, gain_in, 9).start()
    for g in range(GROUPS):
        local(wq_hbm.at[:, q_cols(x, g)], wa.at[g, f, x, c, :, pl.ds(0, qw)], 2 * g).start()
        local(wk_hbm.at[:, k_cols(x, g)], wa.at[g, f, x, c, :, pl.ds(qw, kw)], 2 * g).start()
        local(wv_hbm.at[:, k_cols(x, g)], wv.at[g, f, x, c, pl.ds(0, rows)], 2 * g + 1).start()
    local(wo_hbm.at[:, oa_cols(x)], woa.at[f, x, c], 4).start()
    local(wo_hbm.at[:, ob_cols(x)], wob.at[f, x, c], 5).start()
    local(hid_hbm, hid.at[0], 6).start()
    local(cos_hbm, cos_ref, 7).start()
    local(sin_hbm, sin_ref, 8).start()

    def inverse_rms(t):
        value = hid[t].astype(jnp.float32)
        return lax.rsqrt(jnp.mean(value * value, axis=-1, keepdims=True) + norm_eps)

    barrier = pltpu.get_barrier_semaphore()
    for target in (across, inward, partner, sibling):
        pl.semaphore_signal(barrier, inc=1, device_id=target, device_id_type=MESH)
    pl.when(middle)(lambda: pl.semaphore_signal(
        barrier, inc=1, device_id=outward, device_id_type=MESH))
    acc[...] = jnp.zeros_like(acc)
    local(gain_hbm, gain_in, 9).wait()
    gain = gain_in[...].astype(jnp.float32)
    gain = jnp.broadcast_to(jnp.concatenate([gain, gain], axis=1), (16, LANES))
    gain_tile[...] = gain.astype(jnp.bfloat16)
    for g in range(GROUPS):
        wv[g, f, x, c, rows:rows + 16, :] = gain.astype(jnp.bfloat16)
    local(hid_hbm, hid.at[0], 6).wait()
    inv_own = inverse_rms(0)
    pl.semaphore_wait(barrier, 4 + mine)

    def swap(src, dst, number, sem):
        return pltpu.make_async_remote_copy(
            src_ref=src, dst_ref=dst, send_sem=xsend_sem.at[number], recv_sem=xrecv_sem.at[sem],
            device_id=partner, device_id_type=MESH)

    swaps = []
    for g in range(GROUPS):
        h = 1 - x
        swaps += [
            swap(wq_hbm.at[:, q_cols(h, g)], wa.at[g, f, x, c, :, pl.ds(0, qw)], 0, 2 * g),
            swap(wk_hbm.at[:, k_cols(h, g)], wa.at[g, f, x, c, :, pl.ds(qw, kw)], 0, 2 * g),
            swap(wv_hbm.at[:, k_cols(h, g)], wv.at[g, f, x, c, pl.ds(0, rows)], 1, 2 * g + 1),
            swap(gain_tile, wv.at[g, f, x, c, pl.ds(rows, 16)], 1, 2 * g + 1),
        ]
    swaps.append(swap(hid_hbm, hid.at[1], 2, 6))
    swaps.append(swap(wo_hbm.at[:, oa_cols(1 - x)], woa.at[f, x, c], 3, 4))
    swaps.append(swap(wo_hbm.at[:, ob_cols(1 - x)], wob.at[f, x, c], 4, 5))
    for copy in swaps:
        copy.start()

    def swapped(ref, sem):
        swap(ref, ref, 0, sem).wait_recv()

    def ready(stage, xs):
        part = x if xs == 0 else 1 - x
        if stage < GROUPS:
            refs = ((wa.at[stage, f, part, c], 2 * stage),
                    (wv.at[stage, f, part, c, pl.ds(0, rows + 16 * xs)], 2 * stage + 1))
        else:
            refs = ((woa.at[f, part, c], 4), (wob.at[f, part, c], 5))
        for ref, sem in refs:
            if xs == 0:
                local(ref, ref, sem).wait()
            else:
                swapped(ref, sem)

    def stretch(number, cond=None):
        for plan, here, own in ((EDGE_PLAN, edge, 0), (MIDDLE_PLAN, middle, 1)):
            if plan[number]:
                def run(plan=plan, own=own):
                    for code in plan[number]:
                        if code < 100:
                            relay(code, own)
                        else:
                            stage, xs = (code - 100) // 2, (code - 100) % 2
                            ready(stage, xs)
                            kinds = ("a", "b") if stage < GROUPS else ("oa", "ob")
                            origin_ways(kinds, stage % GROUPS, x if xs == 0 else 1 - x, own)
                pl.when(here if cond is None else here & cond)(run)

    def stretches(first, step, count):
        for number in range(count):
            stretch(first + number, step == number)

    def gain_row(zs):
        lane = lax.broadcasted_iota(jnp.int32, (1, LANES), 1)
        parts = []
        for col in range(2):
            for xs in range(2):
                low = wv[0, zs * 2 + col, xs, 0, rows:rows + 16, :].astype(jnp.float32)[0:1]
                high = wv[0, zs * 2 + col, xs, 1, rows:rows + 16, :].astype(jnp.float32)[0:1]
                parts.append(jnp.where(lane < rows, low, high))
        return jnp.concatenate(parts, axis=1)

    def normalize(t, zs, inv):
        cols = pl.ds(pl.multiple_of(zs * span, LANES), span)
        value = hid[t, :, cols].astype(jnp.float32) * inv * gain_row(zs)
        nrm[pl.ds(t * tokens, tokens), cols] = value.astype(jnp.bfloat16)

    def project(t, g, zs):
        cols = pl.ds(pl.multiple_of(zs * span, LANES), span)
        left = nrm[pl.ds(t * tokens, tokens), cols]
        fs = pl.ds(zs * 2, 2)
        weight = jnp.concatenate(
            [wa[g, fs].reshape(span, qw + kw), wv[g, fs, :, :, 0:rows, :].reshape(span, kw)], axis=1)
        acc[g, pl.ds(t * tokens, tokens), :] += jnp.dot(
            left, weight, preferred_element_type=jnp.float32)

    def attend(g, t):
        base = t * tokens
        span_rows = pl.ds(base, tokens)
        lane = lax.broadcasted_iota(jnp.int32, (tokens, LANES), 1)
        first = lane % HD < HD // 2
        left_head = lane < HD

        def turn(tile):
            turned = jnp.where(first, pltpu.roll(tile, LANES - HD // 2, 1),
                               pltpu.roll(tile, HD // 2, 1))
            return tile * cos_ref[...] + turned * sin_ref[...]

        key = turn(acc[g, span_rows, qw:qw + kw])
        value = acc[g, span_rows, qw + kw:qw + 2 * kw]
        key_other, value_other = pltpu.roll(key, HD, 1), pltpu.roll(value, HD, 1)
        heads = qw // (kw // HD)
        block = tokens // 2
        wide = heads // LANES * block
        key_at = lax.broadcasted_iota(jnp.int32, (block, wide), 0)
        open_ = lax.broadcasted_iota(jnp.int32, (block, wide), 1) % block >= key_at
        for j in range(kw // HD):
            def low_high(tile, tile_other):
                low = tile if j == 0 else tile_other
                high = tile_other if j == 0 else tile
                zero = jnp.zeros_like(tile)
                return (jnp.where(left_head, low, zero).astype(jnp.bfloat16),
                        jnp.where(left_head, zero, high).astype(jnp.bfloat16))

            key_low, key_high = low_high(key, key_other)
            value_low, value_high = low_high(value, value_other)
            query = []
            for p in range(heads // LANES):
                at = j * heads + p * LANES
                tile = turn(acc[g, span_rows, at:at + LANES])
                query.append(tile.astype(jnp.bfloat16) * jnp.bfloat16(HD ** -0.5))
            for b in range(2):
                seen = (b + 1) * block
                stacked = jnp.concatenate([q[b * block:seen] for q in query], axis=0)
                keys = jnp.concatenate([key_low[:seen], key_high[:seen]], axis=0)
                values = jnp.concatenate([value_low[:seen], value_high[:seen]], axis=0)
                scores = lax.dot_general(keys, stacked, NT, preferred_element_type=jnp.float32)
                probs = []
                for e in range(2):
                    begin, end = e * seen, (e + 1) * seen
                    part = jnp.where(open_, scores[end - block:end], -1e30)
                    if b > 0:
                        part = jnp.concatenate([scores[begin:end - block], part], axis=0)
                    expo = jnp.exp(part - jnp.max(part, axis=0, keepdims=True))
                    total = jnp.sum(expo, axis=0, keepdims=True)
                    probs.append((expo * (1.0 / total)).astype(jnp.bfloat16))
                mixed = lax.dot_general(jnp.concatenate(probs, axis=0), values, TN,
                                        preferred_element_type=jnp.float32).astype(jnp.bfloat16)
                for p in range(heads // LANES):
                    at = g * qw + j * heads + p * LANES
                    ctx[pl.ds(base + b * block, block), at:at + LANES] = (
                        mixed[p * block:(p + 1) * block])

    def place(n):
        col, k = (jnp.where(edge, OTHER_ORDER[0][n][which], OTHER_ORDER[1][n][which])
                  for which in range(2))
        return at_line(k) * 2 + jnp.where(col == 0, y, 1 - y)

    def block_cols(fs):
        return pl.ds(pl.multiple_of(fs * piece_cols, LANES), piece_cols)

    def out_part(fs):
        weight = jnp.concatenate([woa[fs].reshape(piece_cols, cut),
                                  wob[fs].reshape(piece_cols, half_out - cut)], axis=1)
        return lax.dot_general(ctx[tokens:2 * tokens, :], weight, NT,
                               preferred_element_type=jnp.float32)

    def out_other(n):
        fs = place(n)
        for kind in ("oa", "ob"):
            ref = view(kind, 0, fs, 1 - c)
            pltpu.make_async_remote_copy(
                src_ref=ref, dst_ref=ref, send_sem=send_sem.at[0, 3],
                recv_sem=sibo_sem.at[index(kind, 0) - 2 * GROUPS, fs], device_id=sibling,
                device_id_type=MESH).wait_recv()
        psend[fs] = out_part(fs).astype(jnp.bfloat16)
        pltpu.make_async_remote_copy(
            src_ref=psend.at[fs], dst_ref=other_out.at[:, block_cols(fs)], send_sem=psend_sem,
            recv_sem=precv_sem, device_id=partner, device_id_type=MESH).start()

    def out_own(n):
        zs = picked(n, OWN_ORDER)
        both = pl.ds(zs * 2, 2)
        weight = jnp.concatenate([woa[both].reshape(span, cut),
                                  wob[both].reshape(span, half_out - cut)], axis=1)
        part = lax.dot_general(ctx[0:tokens, :], weight, NT, preferred_element_type=jnp.float32)
        cols = pl.ds(pl.multiple_of(zs * span, LANES), span)
        own[zs] = hid[0, :, cols].astype(jnp.float32) + part
        pltpu.make_async_copy(own.at[zs], own_out.at[:, cols], own_sem).start()

    def own_first(i, carry):
        stretches(0, i, Z_LINE)
        zs = picked(i, FIRST_ORDER)
        sibling_arrived(("a", "b"), 0, zs)
        normalize(0, zs, inv_own)
        project(0, 0, zs)
        return carry

    lax.fori_loop(0, Z_LINE, own_first, 0)
    local(cos_hbm, cos_ref, 7).wait()
    local(sin_hbm, sin_ref, 8).wait()
    stretch(4)
    attend(0, 0)
    stretch(5)
    swap(hid_hbm, hid.at[1], 2, 6).wait_recv()
    inv_other = inverse_rms(1)

    def other_first(i, carry):
        stretches(6, i, Z_LINE)
        normalize(1, i, inv_other)
        project(1, 0, i)
        return carry

    lax.fori_loop(0, Z_LINE, other_first, 0)
    stretch(10)
    attend(0, 1)

    def other_second(i, carry):
        stretches(11, i, Z_LINE)
        zs = picked(i, SECOND_ORDER)
        sibling_arrived(("a", "b"), 1, zs)
        project(1, 1, zs)
        return carry

    lax.fori_loop(0, Z_LINE, other_second, 0)
    stretch(15)
    attend(1, 1)
    stretch(16)
    out_other(0)
    stretch(17)
    out_other(1)

    def own_second(i, carry):
        stretches(18, i, Z_LINE)
        project(0, 1, i)
        return carry

    lax.fori_loop(0, Z_LINE, own_second, 0)
    stretch(22)
    out_other(2)
    stretch(23)
    out_other(3)
    stretch(24)
    attend(1, 0)
    stretch(25)
    out_other(4)
    stretch(26)
    out_own(0)
    stretch(27)
    out_other(5)
    stretch(28)
    out_own(1)
    stretch(29)
    out_other(6)
    stretch(30)
    out_own(2)
    stretch(31)
    out_other(7)
    stretch(32)
    out_own(3)
    for number in range(33, len(EDGE_PLAN)):
        stretch(number)

    for number, ref in enumerate((wa.at[:, f, 0, c], wv.at[:, f, 0, c], hid.at[1],
                                  woa.at[f, 0, c], wob.at[f, 0, c])):
        swap(ref, ref, number, 0).wait_send()
    sent("sibling", 2 * Z_LINE, 2 * Z_LINE)
    sent("across", Z_LINE, 1)
    pl.when(edge)(lambda: sent("inward", 1, 2))

    @pl.when(middle)
    def _():
        sent("inward", 2, 4)
        sent("outward", 3, 6)

    pltpu.make_async_copy(own, own, own_sem).wait()
    everything = pltpu.make_async_remote_copy(
        src_ref=psend, dst_ref=psend, send_sem=psend_sem, recv_sem=precv_sem, device_id=partner,
        device_id_type=MESH)
    everything.wait_send()
    everything.wait_recv()


def fused(hidden, attn_gain, w_query, w_key, w_value, w_out):
    tokens, width = hidden.shape
    rows, width_query = w_query.shape
    width_kv = w_key.shape[1]
    fsdp = Z_LINE * 2
    qw, kw = width_query // 2 // GROUPS, width_kv // 2 // GROUPS
    half_out = width_query // 2
    span = width // Z_LINE
    cos_table, sin_table = lane_tables(tokens)
    kinds = 2 * GROUPS + 2
    dma = pltpu.SemaphoreType.DMA
    own, other = pl.pallas_call(
        block_kernel,
        out_shape=(jax.ShapeDtypeStruct((tokens, width), jnp.float32),
                   jax.ShapeDtypeStruct((tokens, width), jnp.bfloat16)),
        in_specs=[pl.BlockSpec(memory_space=pl.ANY)] * 8,
        out_specs=(pl.BlockSpec(memory_space=pl.ANY), pl.BlockSpec(memory_space=pl.ANY)),
        scratch_shapes=[
            pltpu.VMEM((GROUPS, fsdp, 2, 2, rows, qw + kw), jnp.bfloat16),
            pltpu.VMEM((GROUPS, fsdp, 2, 2, rows + 16, kw), jnp.bfloat16),
            pltpu.VMEM((fsdp, 2, 2, rows, half_out - LANES), jnp.bfloat16),
            pltpu.VMEM((fsdp, 2, 2, rows, LANES), jnp.bfloat16),
            pltpu.VMEM((2, tokens, width), jnp.bfloat16),
            pltpu.VMEM((2 * tokens, width), jnp.bfloat16),
            pltpu.VMEM((GROUPS, 2 * tokens, qw + 2 * kw), jnp.float32),
            pltpu.VMEM((2 * tokens, half_out), jnp.bfloat16),
            pltpu.VMEM((tokens, LANES), jnp.float32),
            pltpu.VMEM((tokens, LANES), jnp.float32),
            pltpu.VMEM((fsdp, tokens, 4 * rows), jnp.bfloat16),
            pltpu.VMEM((Z_LINE, tokens, span), jnp.float32),
            pltpu.VMEM((1, rows), jnp.bfloat16),
            pltpu.VMEM((16, LANES), jnp.bfloat16),
            dma((len(BUFFERS), 4)),
            dma((kinds, fsdp)),
            dma((2 * GROUPS, Z_LINE)),
            dma((2, fsdp)),
            dma((5,)),
            dma((7,)),
            dma((10,)),
            dma,
            dma,
            dma,
        ],
        compiler_params=pltpu.CompilerParams(
            collective_id=0, has_side_effects=True, vmem_limit_bytes=40 * 1024 * 1024),
        name="attention_block",
    )(*[pltpu.with_memory_space_constraint(value, pltpu.HBM) for value in (
        hidden, attn_gain[None, :], w_query, w_key, w_value, w_out.T,
        jnp.asarray(cos_table), jnp.asarray(sin_table))])
    return (own + other.astype(jnp.float32)).astype(hidden.dtype)


def fits(fsdp, rep, hidden, w_query, w_key, w_out):
    tokens, width = hidden.shape
    rows, width_query = w_query.shape
    return (
        rep == 4
        and fsdp == 2 * Z_LINE
        and 2 * rows == LANES
        and width == fsdp * rep * rows
        and w_out.shape == (width_query, rows)
        and w_key.shape[1] == 2 * GROUPS * LANES
        and width_query == 4 * w_key.shape[1]
        and tokens % LANES == 0
    )


def body(fsdp, rep, hidden, attn_gain, w_query, w_key, w_value, w_out):
    if fits(fsdp, rep, hidden, w_query, w_key, w_out):
        return fused(hidden, attn_gain, w_query, w_key, w_value, w_out)
    tokens = hidden.shape[0]
    head_dim = HD
    width_query = w_query.shape[1]
    width_kv = w_key.shape[1]
    kv_count = width_kv // head_dim
    group = width_query // width_kv
    x_float = hidden.astype(jnp.float32)
    inv_rms = lax.rsqrt(jnp.mean(x_float * x_float, axis=-1, keepdims=True) + norm_eps)
    width_rows = w_query.shape[0]
    packed = jnp.concatenate(
        [w_query, w_key, w_value, w_out.T, jnp.broadcast_to(attn_gain[:, None], (width_rows, 128))],
        axis=1,
    )
    packed = lax.all_gather(packed, ("fsdp", "rep"), axis=0, tiled=True)
    cut_key = width_query
    cut_value = cut_key + width_kv
    cut_out = cut_value + width_kv
    cut_gain = cut_out + w_out.shape[0]
    query_piece = packed[:, :cut_key]
    key_piece = packed[:, cut_key:cut_value]
    value_piece = packed[:, cut_value:cut_out]
    out_piece = packed[:, cut_out:cut_gain]
    gain_piece = packed[:, cut_gain]
    normed = (x_float * inv_rms * gain_piece.astype(jnp.float32)[None, :]).astype(jnp.bfloat16)
    queries = jnp.dot(normed, query_piece, preferred_element_type=jnp.float32)
    keys_raw = jnp.dot(normed, key_piece, preferred_element_type=jnp.float32)
    values_raw = jnp.dot(normed, value_piece, preferred_element_type=jnp.float32)
    cos_table, sin_table = rope_tables(tokens, head_dim)
    queries = queries.reshape(tokens, kv_count, group, head_dim)
    keys_raw = keys_raw.reshape(tokens, kv_count, head_dim)
    values_bf = values_raw.reshape(tokens, kv_count, head_dim).astype(jnp.bfloat16)
    rope_queries = rotate(queries, cos_table[:, None, None, :], sin_table[:, None, None, :]).astype(
        jnp.bfloat16
    )
    rope_keys = rotate(keys_raw, cos_table[:, None, :], sin_table[:, None, :]).astype(jnp.bfloat16)
    scores = jnp.einsum(
        "qkgd,skd->kgqs", rope_queries, rope_keys, preferred_element_type=jnp.float32
    ) * head_dim ** (-0.5)
    causal = jnp.arange(tokens)[:, None] >= jnp.arange(tokens)[None, :]
    scores = jnp.where(causal[None, None, :, :], scores, -1e30)
    top = jnp.max(scores, axis=-1, keepdims=True)
    expo = jnp.exp(scores - top)
    probs = (expo / jnp.sum(expo, axis=-1, keepdims=True)).astype(jnp.bfloat16)
    context = jnp.einsum("kgqs,skd->qkgd", probs, values_bf, preferred_element_type=jnp.float32)
    context = context.reshape(tokens, width_query).astype(jnp.bfloat16)
    branch = lax.dot_general(
        context, out_piece, (((1,), (1,)), ((), ())), preferred_element_type=jnp.float32
    )
    return (x_float + branch).astype(jnp.bfloat16)


def solution(mesh):
    placed = (
        P(("fsdp", "rep"), None),
        P(("fsdp", "rep")),
        P(("fsdp", "rep"), None),
        P(("fsdp", "rep"), None),
        P(("fsdp", "rep"), None),
        P(None, ("fsdp", "rep")),
    )
    return jax.shard_map(
        functools.partial(body, mesh.shape["fsdp"], mesh.shape["rep"]),
        mesh=mesh,
        in_specs=placed,
        out_specs=P(("fsdp", "rep"), None),
        check_vma=False,
    )
```
